128 devices in a mesh: cuts: 32 (over y, z, core), tile: 4 (over x).
Axes of the slice: x: 4, y: 4, z: 4, core: 2. Of those that a mesh axis runs over, the one named last changes fastest.
Arguments:
- probe_wave: float32 [2, 256, 256], replicated, may hold values from -6 to 6
- object_field: bfloat16 [2, 32, 512, 512], P(None, 'cuts', 'tile'), may hold values from -1.03 to 1.03, as said below
- pos_rows: int32 [16], P('tile'), may hold values from 0 to 256
- pos_cols: int32 [16], P('tile'), may hold values from 0 to 256
- intensity: float32 [16, 256, 256], P('tile'), may hold values from 0.05 to 2
- prop_phase: float32 [256, 256], replicated, may hold values from -3.140625 to 3.140625
Outputs:
- object_grad: float32 [2, 32, 512, 512], P(None, 'cuts', 'tile')
The draws below stay inside these ranges and needn't reach their ends.
Inputs may be any that keep to these rules, and one draw needn't show every extreme that they name: `object_field`: each slice's transmission has magnitude between 0.95 and 1.025.
All inputs are finite; a program needn't handle non-finite values.
Results may differ from the reference program's by a relative error of at most 0.0003.
Values may be sent and summed in bfloat16 or wider, within the bound.
No kernel may reach another device: no remote copies, remote signals or barrier semaphores. Data moves between devices by JAX's collectives and lax.ppermute only.
A program may use at most 64 MiB of HBM per device.

```python
import math
import jax
import jax.numpy as jnp
from jax import lax

WIN = 256
W = 512
SLICES = 32
H = 512
POSITIONS = 16


def draw_object_field(key, part):
    key_amp, key_phase = jax.random.split(jax.random.fold_in(key, 11))
    amplitude = jax.random.uniform(key_amp, (SLICES, H, W), jnp.float32, 0.95, 1.025)
    phases = 0.4 * jax.random.truncated_normal(key_phase, -2.5, 2.5, (SLICES, H, W), jnp.float32)
    return jnp.stack([amplitude * jnp.cos(phases), amplitude * jnp.sin(phases)]).astype(jnp.bfloat16)


def place_ends(values, key, least, high):
    longest = values.shape.index(max(values.shape))
    spots = []
    for shift in (0, 1):
        where = [jax.random.randint(jax.random.fold_in(key, axis), (), 0, length) for axis, length in enumerate(values.shape)]
        where[longest] = (where[longest] + shift) % values.shape[longest]
        spots.append(tuple(where))
    return values.at[spots[0]].set(least).at[spots[1]].set(high)


def block_scale(key, extent, cuts, low, high):
    factor_of, own = 1.0, jax.random.fold_in(key, 6)
    for dim, blocks in cuts:
        draws = jnp.exp(jax.random.uniform(jax.random.fold_in(own, dim), (blocks,), jnp.float32, low / len(cuts), high / len(cuts)))
        factor_of = factor_of * jnp.repeat(draws, extent[dim] // blocks).reshape([-1 if axis == dim else 1 for axis in range(len(extent))])
    return factor_of


def centred(key, shape, scale, reach, kind=jnp.bfloat16):
    drawn = jax.random.normal(key, shape, jnp.float32) * scale
    return jnp.minimum(jnp.maximum(drawn, -reach), reach).astype(kind)


def setup_inputs(seed: int = 0) -> dict:
    keys = jax.random.split(jax.random.key(seed), 7)
    return {
        "probe_wave": centred(keys[0], (2, WIN, WIN), 1.0, 6.0, jnp.float32),
        "object_field": draw_object_field(jax.random.fold_in(keys[6], 71), 0),
        "pos_rows": place_ends(jax.random.randint(keys[2], (POSITIONS,), 0, H - WIN + 1), jax.random.fold_in(keys[2], 1), 0, H - WIN).astype(jnp.int32),
        "pos_cols": place_ends(jax.random.randint(keys[3], (POSITIONS,), 0, W - WIN + 1), jax.random.fold_in(keys[3], 1), 0, W - WIN).astype(jnp.int32),
        "intensity": jnp.clip(jnp.exp(math.log(2.0) - 3.6888794 * jax.random.uniform(keys[4], (POSITIONS, WIN, WIN), jnp.float32) ** block_scale(keys[4], (POSITIONS, WIN, WIN), ((0, 4),), -0.2, 0.2)), 0.05, 2.0),
        "prop_phase": jnp.clip(jax.random.uniform(keys[5], (WIN, WIN), jnp.float32, -3.140625, 3.140625), -3.140625, 3.140625),
    }


def dft_tables(win_size):
    indices = jnp.arange(win_size, dtype=jnp.int32)
    products = indices[:, None] * indices[None, :] % win_size
    angles = products.astype(jnp.float32) * (2.0 * math.pi / win_size)
    norm_scale = 1.0 / math.sqrt(win_size)
    return jnp.stack([jnp.cos(angles) * norm_scale, jnp.sin(angles) * norm_scale]).astype(jnp.float32)

def transform(field, tables, sign_flip):
    left_prod = jnp.einsum('tjk,...ckl->...tcjl', tables, field, precision=lax.Precision.HIGHEST)
    half_real = left_prod[..., 0, 0, :, :] + sign_flip * left_prod[..., 1, 1, :, :]
    half_imag = left_prod[..., 0, 1, :, :] - sign_flip * left_prod[..., 1, 0, :, :]
    half = jnp.stack([half_real, half_imag], axis=-3)
    right_prod = jnp.einsum('...cjk,tkl->...ctjl', half, tables, precision=lax.Precision.HIGHEST)
    out_real = right_prod[..., 0, 0, :, :] + sign_flip * right_prod[..., 1, 1, :, :]
    out_imag = right_prod[..., 1, 0, :, :] - sign_flip * right_prod[..., 0, 1, :, :]
    return jnp.stack([out_real, out_imag], axis=-3)

def slice_step(in_wave, obj_layer, tables, prop_cos, prop_sin):
    mixed_real = in_wave[..., 0, :, :] * obj_layer[..., 0, :, :] - in_wave[..., 1, :, :] * obj_layer[..., 1, :, :]
    mixed_imag = in_wave[..., 0, :, :] * obj_layer[..., 1, :, :] + in_wave[..., 1, :, :] * obj_layer[..., 0, :, :]
    mixed_wave = jnp.stack([mixed_real, mixed_imag], axis=-3)
    spectrum = transform(mixed_wave, tables, 1.0)
    spread_real = spectrum[..., 0, :, :] * prop_cos - spectrum[..., 1, :, :] * prop_sin
    spread_imag = spectrum[..., 0, :, :] * prop_sin + spectrum[..., 1, :, :] * prop_cos
    spread = jnp.stack([spread_real, spread_imag], axis=-3)
    return transform(spread, tables, -1.0)

def farfield_loss(exit_wave, measured, tables):
    spectrum = transform(exit_wave, tables, 1.0)
    magnitude = spectrum[..., 0, :, :] * spectrum[..., 0, :, :] + spectrum[..., 1, :, :] * spectrum[..., 1, :, :]
    return 0.5 * jnp.sum((magnitude - measured) ** 2)

def reference(probe_wave, object_field, pos_rows, pos_cols, intensity, prop_phase):
    tables = dft_tables(WIN)
    prop_cos = jnp.cos(prop_phase)
    prop_sin = jnp.sin(prop_phase)
    grad_region = jnp.zeros(object_field.shape, jnp.float32)
    zero_index = jnp.zeros((), jnp.int32)

    def one_position(grad_region, pos_slot):
        row_at = lax.dynamic_index_in_dim(pos_rows, pos_slot, 0, keepdims=False).astype(jnp.int32)
        col_at = lax.dynamic_index_in_dim(pos_cols, pos_slot, 0, keepdims=False).astype(jnp.int32)
        start = (zero_index, zero_index, row_at, col_at)
        patch = lax.dynamic_slice(object_field, start, (2, SLICES, WIN, WIN)).astype(jnp.float32)
        layers = jnp.transpose(patch, (1, 0, 2, 3))
        measured = lax.dynamic_index_in_dim(intensity, pos_slot, 0, keepdims=False)

        def loss_of(layers):

            def slice_turn(in_wave, obj_layer):
                return (slice_step(in_wave, obj_layer, tables, prop_cos, prop_sin).astype(jnp.float32), None)
            last_wave, _ = lax.scan(slice_turn, probe_wave.astype(jnp.float32), layers)
            return farfield_loss(last_wave, measured, tables)
        patch_grad = jnp.transpose(jax.grad(loss_of)(layers), (1, 0, 2, 3)).astype(jnp.float32)
        current = lax.dynamic_slice(grad_region, start, (2, SLICES, WIN, WIN))
        return (lax.dynamic_update_slice(grad_region, current + patch_grad, start), None)
    grad_region, _ = lax.scan(one_position, grad_region, jnp.arange(POSITIONS, dtype=jnp.int32))
    return grad_region
```

```python
import math

import jax
import jax.numpy as jnp
import ml_dtypes
import numpy as np
from jax import lax
from jax.experimental import pallas as pl
from jax.experimental.pallas import tpu as pltpu
from jax.sharding import Mesh, PartitionSpec as P

N = 256
M = N // 2
F32 = jnp.float32
BF16 = jnp.bfloat16


def tables():
    half = np.arange(M) + 0.5
    angles = 2.0 * math.pi / N * half[:, None] * half[None, :]
    packed, gain = [], []
    for values in (np.cos(angles) / 16.0, np.sin(angles) / 16.0):
        high = values.astype(ml_dtypes.bfloat16)
        low = (values - high.astype(np.float64)).astype(ml_dtypes.bfloat16)
        packed.append(np.block([[high, low], [high, low]]))
        both = high.astype(np.float64) + low.astype(np.float64)
        gain.append(4.0 * np.trace(both @ both) / M)
    return packed[0], packed[1], np.ascontiguousarray(packed[0].T), np.ascontiguousarray(packed[1].T), float(np.mean(gain)) ** 2


def split(x):
    high = x.astype(BF16)
    return high, (x - high.astype(F32)).astype(BF16)


def dot(a, b):
    return jnp.dot(a, b, preferred_element_type=F32)


def right(blocks, table):
    high, low = split(jnp.concatenate(blocks, axis=0))
    out = dot(jnp.concatenate([high, low], axis=1), table)
    out = out[:, :M] + out[:, M:]
    return [out[i * M : (i + 1) * M] for i in range(4)]


def left(blocks, table):
    high, low = split(jnp.concatenate(blocks, axis=1))
    out = dot(table, jnp.concatenate([high, low], axis=0))
    out = out[:M] + out[M:]
    return [out[:, i * M : (i + 1) * M] for i in range(4)]


def spectrum(quads, tabs):
    folded = []
    for x11, x12, x21, x22 in quads:
        d1, d2, s1, s2 = x11 - x21, x12 - x22, x11 + x21, x12 + x22
        folded.append((d1 - d2, d1 + d2, s1 - s2, s1 + s2))
    (ddr, dsr, sdr, ssr), (ddi, dsi, sdi, ssi) = folded
    cos_r, sin_r, cos_l, sin_l = tabs
    ddr, sdr, ddi, sdi = right([ddr, sdr, ddi, sdi], cos_r)
    dsr, ssr, dsi, ssi = right([dsr, ssr, dsi, ssi], sin_r)
    ppr, pqr, ppi, pqi = left([ddr, dsr, ddi, dsi], cos_l)
    qpr, qqr, qpi, qqi = left([sdr, ssr, sdi, ssi], sin_l)
    ar, ai, br, bi = ppr - qqr, ppi - qqi, ppr + qqr, ppi + qqi
    er, ei, gr, gi = pqr + qpr, pqi + qpi, pqr - qpr, pqi - qpi
    real = (ar + ei, br - gi, br + gi, ar - ei)
    imag = (ai - er, bi + gr, bi - gr, ai + er)
    return real, imag


def wave_of(spec, tabs):
    cos_r, sin_r, cos_l, sin_l = tabs
    (yr11, yr12, yr21, yr22), (yi11, yi12, yi21, yi22) = spec
    apr, api, amr, ami = yr11 + yr22, yi11 + yi22, yr11 - yr22, yi11 - yi22
    bpr, bpi, bmr, bmi = yr12 + yr21, yi12 + yi21, yr12 - yr21, yi12 - yi21
    ppr, ppi, qqr, qqi = apr + bpr, api + bpi, bpr - apr, bpi - api
    pqr, pqi = bmi - ami, amr - bmr
    qpr, qpi = -(ami + bmi), amr + bmr
    ppr, pqr, ppi, pqi = left([ppr, pqr, ppi, pqi], cos_l)
    qpr, qqr, qpi, qqi = left([qpr, qqr, qpi, qqi], sin_l)
    uur, vur, uui, vui = right([ppr, qpr, ppi, qpi], cos_r)
    uvr, vvr, uvi, vvi = right([pqr, qqr, pqi, qqi], sin_r)
    quads = []
    for uu, uv, vu, vv in ((uur, uvr, vur, vvr), (uui, uvi, vui, vvi)):
        p1, m1, p2, m2 = vv + uu, vv - uu, vu + uv, vu - uv
        quads.append((p1 + p2, m1 - m2, m1 + m2, p1 - p2))
    return quads


def quarters(ref, *lead):
    return tuple(ref[(*lead, slice(i * M, i * M + M), slice(j * M, j * M + M))] for i in (0, 1) for j in (0, 1))


def put(ref, quads, *lead):
    for part in (0, 1):
        for at, value in enumerate(quads[part]):
            i, j = divmod(at, 2)
            ref[(*lead, part, slice(i * M, i * M + M), slice(j * M, j * M + M))] = value


def times(ar, ai, br, bi):
    real = tuple(w * x - y * z for w, x, y, z in zip(ar, br, ai, bi))
    imag = tuple(w * z + y * x for w, x, y, z in zip(ar, br, ai, bi))
    return real, imag


def conj_times(ar, ai, br, bi):
    real = tuple(w * x + y * z for w, x, y, z in zip(ar, br, ai, bi))
    imag = tuple(w * z - y * x for w, x, y, z in zip(ar, br, ai, bi))
    return real, imag


def as_f32(values):
    return tuple(v.astype(F32) for v in values)


def forward_kernel(gain, is_last, steps, mine_ref, obj_ref, wave_ref, prop_ref, cr, sr, cl, sl, *rest):
    if is_last:
        inten_ref, out_ref, kept_ref = rest
    else:
        out_ref, kept_ref = rest
    step = pl.program_id(0)
    tabs = (cr[...], sr[...], cl[...], sl[...])

    @pl.when(step == 0)
    def _():
        out_ref[...] = wave_ref[...]

    @pl.when(step == mine_ref[0])
    def _():
        kept_ref[...] = out_ref[...]

    objr, obji = as_f32(quarters(obj_ref, 0, 0)), as_f32(quarters(obj_ref, 0, 1))
    mixed = times(quarters(out_ref, 0), quarters(out_ref, 1), objr, obji)
    spec = spectrum(mixed, tabs)
    spread = times(spec[0], spec[1], quarters(prop_ref, 0), quarters(prop_ref, 1))
    put(out_ref, wave_of(spread, tabs))

    if is_last:

        @pl.when(step == steps - 1)
        def _():
            real, imag = spectrum((quarters(out_ref, 0), quarters(out_ref, 1)), tabs)
            scale = [(2.0 / gain) * (x * x + y * y - z) for x, y, z in zip(real, imag, quarters(inten_ref))]
            slope = tuple(s * x for s, x in zip(scale, real)), tuple(s * x for s, x in zip(scale, imag))
            put(out_ref, wave_of(slope, tabs))


def paired_index(shape, axis):
    at = lax.broadcasted_iota(jnp.int32, shape, axis)
    return jnp.where(at < M, at, N + M - 1 - at)


def chosen(start, shape, window_axis):
    window = paired_index(shape, window_axis) + start
    return jnp.where(window == lax.broadcasted_iota(jnp.int32, shape, 1 - window_axis), 1.0, 0.0).astype(BF16)


def backward_kernel(steps, width, height, scalars, obj_ref, ct_ref, prop_ref, cr, sr, cl, sl, kept_ref, out_ref, region_ref, grad_ref):
    step = pl.program_id(0)
    tabs = (cr[...], sr[...], cl[...], sl[...])

    @pl.when(step == 0)
    def _():
        out_ref[...] = ct_ref[...]

    spec = spectrum((quarters(out_ref, 0), quarters(out_ref, 1)), tabs)
    back = conj_times(quarters(prop_ref, 0), quarters(prop_ref, 1), spec[0], spec[1])
    put(out_ref, wave_of(back, tabs))

    @pl.when(steps - 1 - step == scalars[0])
    def _():
        ct = quarters(out_ref, 0), quarters(out_ref, 1)
        put(grad_ref, conj_times(quarters(kept_ref, 0), quarters(kept_ref, 1), ct[0], ct[1]))

    objr, obji = as_f32(quarters(obj_ref, 0, 0)), as_f32(quarters(obj_ref, 0, 1))
    put(out_ref, conj_times(objr, obji, quarters(out_ref, 0), quarters(out_ref, 1)))

    @pl.when(step == steps - 1)
    def _():
        rows = chosen(scalars[1], (height, N), 1)
        cols = chosen(scalars[2], (N, width), 0)
        for part in (0, 1):
            high, low = split(grad_ref[part])
            spread = [dot(rows, dot(x, cols).astype(BF16)) for x in (high, low)]
            region_ref[part] = spread[0] + spread[1]


def cut_kernel(rows_ref, cols_ref, obj_ref, out_ref):
    height, width = obj_ref.shape[-2:]
    at = pl.program_id(0)
    rows = chosen(rows_ref[at], (N, height), 0)
    cols = chosen(cols_ref[at], (width, N), 1)
    for part in (0, 1):
        out_ref[0, part] = dot(dot(rows, obj_ref[part, 0]).astype(BF16), cols).astype(BF16)


def whole(shape):
    return pl.BlockSpec(shape, lambda *_: (0,) * len(shape))


SMEM = pl.BlockSpec(memory_space=pltpu.SMEM)
PARAMS = pltpu.CompilerParams(dimension_semantics=("arbitrary",), vmem_limit_bytes=48 << 20)
WAVE = (2, N, N)


def cut(full, pos_rows, pos_cols):
    count = pos_rows.shape[0]
    return pl.pallas_call(
        cut_kernel,
        grid=(count,),
        in_specs=[SMEM, SMEM, whole(full.shape)],
        out_specs=pl.BlockSpec((1, 2, N, N), lambda i: (i, 0, 0, 0)),
        out_shape=jax.ShapeDtypeStruct((count, 2, N, N), BF16),
        compiler_params=PARAMS,
        name="cut",
    )(pos_rows, pos_cols, full)


def run_forward(mine, chunk, wave, prop, tabs, gain, inten=None):
    steps = chunk.shape[0]
    last = inten is not None
    extra = (inten,) if last else ()

    def body(*refs):
        forward_kernel(gain, last, steps, *refs)

    return pl.pallas_call(
        body,
        grid=(steps,),
        in_specs=[SMEM, pl.BlockSpec((1, 2, N, N), lambda i: (i, 0, 0, 0)), whole(WAVE), whole(WAVE)]
        + [whole((N, N))] * (4 + len(extra)),
        out_specs=[whole(WAVE), whole(WAVE)],
        out_shape=[jax.ShapeDtypeStruct(WAVE, F32)] * 2,
        compiler_params=PARAMS,
        name="forward",
    )(mine, chunk, wave, prop, *tabs, *extra)


def run_backward(scalars, chunk, ct, prop, tabs, kept, height, width):
    steps = chunk.shape[0]

    def body(*refs):
        backward_kernel(steps, width, height, *refs)

    return pl.pallas_call(
        body,
        grid=(steps,),
        in_specs=[SMEM, pl.BlockSpec((1, 2, N, N), lambda i: (steps - 1 - i, 0, 0, 0)), whole(WAVE), whole(WAVE)]
        + [whole((N, N))] * 4
        + [whole(WAVE)],
        out_specs=[whole(WAVE), whole((2, height, width))],
        out_shape=[jax.ShapeDtypeStruct(WAVE, F32), jax.ShapeDtypeStruct((2, height, width), F32)],
        scratch_shapes=[pltpu.VMEM(WAVE, F32)],
        compiler_params=PARAMS,
        name="backward",
    )(scalars, chunk, ct, prop, *tabs, kept)


def paired(x):
    for axis in (-2, -1):
        first, second = jnp.split(x, 2, axis=axis)
        x = jnp.concatenate([first, jnp.flip(second, axis=axis)], axis=axis)
    return x


def start_wave(probe_wave):
    at = np.arange(N)
    angle = math.pi / N * (at[:, None] + at[None, :])
    cos, sin = np.cos(angle).astype(np.float32), np.sin(angle).astype(np.float32)
    real, imag = probe_wave[0], probe_wave[1]
    return paired(jnp.stack([real * cos - imag * sin, real * sin + imag * cos]))


def on_device(probe_wave, object_field, pos_rows, pos_cols, intensity, prop_phase):
    row = lax.axis_index("y")
    mine = lax.axis_index("zc").astype(jnp.int32)
    chunks_count = lax.axis_size("y")
    height = object_field.shape[2] * lax.axis_size("x")
    width = object_field.shape[3]
    full = lax.all_gather(object_field, "x", axis=2, tiled=True)
    patches = cut(full, pos_rows, pos_cols)
    patches = lax.all_to_all(patches, "y", 0, 0, tiled=True)
    chunks = [lax.all_gather(patches[i], "zc", axis=0) for i in range(chunks_count)]

    *tabs, gain = tables()
    tabs = [jnp.asarray(t) for t in tabs]
    prop = paired(jnp.stack([jnp.cos(prop_phase), jnp.sin(prop_phase)]) * (1.0 / gain))
    inten = paired(lax.dynamic_index_in_dim(intensity, row, 0, keepdims=False))
    wave = start_wave(probe_wave)
    mine_at = mine[None]
    scalars = jnp.stack([mine, pos_rows[row], pos_cols[row]])

    kept = []
    for i in range(chunks_count):
        last = i == chunks_count - 1
        wave, saved = run_forward(mine_at, chunks[i], wave, prop, tabs, gain, inten if last else None)
        kept.append(saved)
    pieces = [None] * chunks_count
    for i in reversed(range(chunks_count)):
        wave, region = run_backward(scalars, chunks[i], wave, prop, tabs, kept[i], height, width)
        pieces[i] = lax.psum_scatter(region, ("x", "y"), scatter_dimension=1, tiled=True)
    out = lax.all_to_all(jnp.stack(pieces), "y", 0, 0, tiled=True)
    out = jnp.transpose(out, (1, 0, 2, 3)).reshape(2, 1, object_field.shape[2], width)
    return out


def solution(mesh):
    devices = mesh.devices
    fine = Mesh(devices.reshape(4, devices.shape[0] // 4, devices.shape[1]), ("y", "zc", "x"))
    return jax.shard_map(
        on_device,
        mesh=fine,
        in_specs=(
            P(),
            P(None, ("y", "zc"), "x", None),
            P("x"),
            P("x"),
            P("x", None, None),
            P(),
        ),
        out_specs=P(None, ("y", "zc"), "x", None),
        check_vma=False,
    )
```

```python
import math

import jax
import jax.numpy as jnp
import ml_dtypes
import numpy as np
from jax import lax
from jax.experimental import pallas as pl
from jax.experimental.pallas import tpu as pltpu
from jax.sharding import Mesh, PartitionSpec as P

N = 256
M = N // 2
F32 = jnp.float32
BF16 = jnp.bfloat16


def tables():
    half = np.arange(M) + 0.5
    angles = 2.0 * math.pi / N * half[:, None] * half[None, :]
    packed, gain = [], []
    for values in (np.cos(angles) / 16.0, np.sin(angles) / 16.0):
        high = values.astype(ml_dtypes.bfloat16)
        low = (values - high.astype(np.float64)).astype(ml_dtypes.bfloat16)
        packed.append(np.block([[high, low], [high, low]]))
        both = high.astype(np.float64) + low.astype(np.float64)
        gain.append(4.0 * np.trace(both @ both) / M)
    return packed[0], packed[1], np.ascontiguousarray(packed[0].T), np.ascontiguousarray(packed[1].T), float(np.mean(gain)) ** 2


def split(x):
    high = x.astype(BF16)
    return high, (x - high.astype(F32)).astype(BF16)


def dot(a, b):
    return jnp.dot(a, b, preferred_element_type=F32)


def right(blocks, table):
    high, low = split(jnp.concatenate(blocks, axis=0))
    out = dot(jnp.concatenate([high, low], axis=1), table)
    out = out[:, :M] + out[:, M:]
    return [out[i * M : (i + 1) * M] for i in range(4)]


def left(blocks, table):
    high, low = split(jnp.concatenate(blocks, axis=1))
    out = dot(table, jnp.concatenate([high, low], axis=0))
    out = out[:M] + out[M:]
    return [out[:, i * M : (i + 1) * M] for i in range(4)]


def spectrum(quads, tabs):
    folded = []
    for x11, x12, x21, x22 in quads:
        d1, d2, s1, s2 = x11 - x21, x12 - x22, x11 + x21, x12 + x22
        folded.append((d1 - d2, d1 + d2, s1 - s2, s1 + s2))
    (ddr, dsr, sdr, ssr), (ddi, dsi, sdi, ssi) = folded
    cos_r, sin_r, cos_l, sin_l = tabs
    ddr, sdr, ddi, sdi = right([ddr, sdr, ddi, sdi], cos_r)
    dsr, ssr, dsi, ssi = right([dsr, ssr, dsi, ssi], sin_r)
    ppr, pqr, ppi, pqi = left([ddr, dsr, ddi, dsi], cos_l)
    qpr, qqr, qpi, qqi = left([sdr, ssr, sdi, ssi], sin_l)
    ar, ai, br, bi = ppr - qqr, ppi - qqi, ppr + qqr, ppi + qqi
    er, ei, gr, gi = pqr + qpr, pqi + qpi, pqr - qpr, pqi - qpi
    real = (ar + ei, br - gi, br + gi, ar - ei)
    imag = (ai - er, bi + gr, bi - gr, ai + er)
    return real, imag


def wave_of(spec, tabs):
    cos_r, sin_r, cos_l, sin_l = tabs
    (yr11, yr12, yr21, yr22), (yi11, yi12, yi21, yi22) = spec
    apr, api, amr, ami = yr11 + yr22, yi11 + yi22, yr11 - yr22, yi11 - yi22
    bpr, bpi, bmr, bmi = yr12 + yr21, yi12 + yi21, yr12 - yr21, yi12 - yi21
    ppr, ppi, qqr, qqi = apr + bpr, api + bpi, bpr - apr, bpi - api
    pqr, pqi = bmi - ami, amr - bmr
    qpr, qpi = -(ami + bmi), amr + bmr
    ppr, pqr, ppi, pqi = left([ppr, pqr, ppi, pqi], cos_l)
    qpr, qqr, qpi, qqi = left([qpr, qqr, qpi, qqi], sin_l)
    uur, vur, uui, vui = right([ppr, qpr, ppi, qpi], cos_r)
    uvr, vvr, uvi, vvi = right([pqr, qqr, pqi, qqi], sin_r)
    quads = []
    for uu, uv, vu, vv in ((uur, uvr, vur, vvr), (uui, uvi, vui, vvi)):
        p1, m1, p2, m2 = vv + uu, vv - uu, vu + uv, vu - uv
        quads.append((p1 + p2, m1 - m2, m1 + m2, p1 - p2))
    return quads


def quarters(ref, *lead):
    return tuple(ref[(*lead, slice(i * M, i * M + M), slice(j * M, j * M + M))] for i in (0, 1) for j in (0, 1))


def put(ref, quads, *lead):
    for part in (0, 1):
        for at, value in enumerate(quads[part]):
            i, j = divmod(at, 2)
            ref[(*lead, part, slice(i * M, i * M + M), slice(j * M, j * M + M))] = value


def times(ar, ai, br, bi):
    real = tuple(w * x - y * z for w, x, y, z in zip(ar, br, ai, bi))
    imag = tuple(w * z + y * x for w, x, y, z in zip(ar, br, ai, bi))
    return real, imag


def conj_times(ar, ai, br, bi):
    real = tuple(w * x + y * z for w, x, y, z in zip(ar, br, ai, bi))
    imag = tuple(w * z - y * x for w, x, y, z in zip(ar, br, ai, bi))
    return real, imag


def as_f32(values):
    return tuple(v.astype(F32) for v in values)


def forward_kernel(gain, is_last, steps, mine_ref, obj_ref, wave_ref, prop_ref, cr, sr, cl, sl, *rest):
    if is_last:
        inten_ref, out_ref, kept_ref = rest
    else:
        out_ref, kept_ref = rest
    step = pl.program_id(0)
    tabs = (cr[...], sr[...], cl[...], sl[...])

    @pl.when(step == 0)
    def _():
        out_ref[...] = wave_ref[...]

    @pl.when(step == mine_ref[0])
    def _():
        kept_ref[...] = out_ref[...]

    objr, obji = as_f32(quarters(obj_ref, 0, 0)), as_f32(quarters(obj_ref, 0, 1))
    mixed = times(quarters(out_ref, 0), quarters(out_ref, 1), objr, obji)
    spec = spectrum(mixed, tabs)
    spread = times(spec[0], spec[1], quarters(prop_ref, 0), quarters(prop_ref, 1))
    put(out_ref, wave_of(spread, tabs))

    if is_last:

        @pl.when(step == steps - 1)
        def _():
            real, imag = spectrum((quarters(out_ref, 0), quarters(out_ref, 1)), tabs)
            scale = [(2.0 / gain) * (x * x + y * y - z) for x, y, z in zip(real, imag, quarters(inten_ref))]
            slope = tuple(s * x for s, x in zip(scale, real)), tuple(s * x for s, x in zip(scale, imag))
            put(out_ref, wave_of(slope, tabs))


def paired_index(shape, axis):
    at = lax.broadcasted_iota(jnp.int32, shape, axis)
    return jnp.where(at < M, at, N + M - 1 - at)


def one_hot(a, b):
    return jnp.where(a == b, 1.0, 0.0).astype(BF16)


def iota(shape, axis):
    return lax.broadcasted_iota(jnp.int32, shape, axis)


def backward_kernel(steps, scalars, obj_ref, ct_ref, prop_ref, cr, sr, cl, sl, kept_ref, *rest):
    out_ref, sent_ref, grad_ref = rest[-3:]
    step = pl.program_id(0)
    tabs = (cr[...], sr[...], cl[...], sl[...])

    @pl.when(step == 0)
    def _():
        out_ref[...] = ct_ref[...]

    spec = spectrum((quarters(out_ref, 0), quarters(out_ref, 1)), tabs)
    back = conj_times(quarters(prop_ref, 0), quarters(prop_ref, 1), spec[0], spec[1])
    put(out_ref, wave_of(back, tabs))

    @pl.when(steps - 1 - step == scalars[0])
    def _():
        ct = quarters(out_ref, 0), quarters(out_ref, 1)
        put(grad_ref, conj_times(quarters(kept_ref, 0), quarters(kept_ref, 1), ct[0], ct[1]))

    objr, obji = as_f32(quarters(obj_ref, 0, 0)), as_f32(quarters(obj_ref, 0, 1))
    put(out_ref, conj_times(objr, obji, quarters(out_ref, 0), quarters(out_ref, 1)))

    @pl.when(step == steps - 1)
    def _():
        at = iota((N, N), 0)
        slot = M * (at // 8 % 2) + 8 * (at // 16) + at % 8
        rows = one_hot((paired_index((N, N), 1) + scalars[1]) % N, slot)
        cols = one_hot((paired_index((N, N), 0) + scalars[2]) % N, iota((N, N), 1))
        for part in (0, 1):
            high, low = split(grad_ref[part])
            rolled = [dot(rows, dot(x, cols).astype(BF16)) for x in (high, low)]
            sent_ref[:, 0, part] = (rolled[0] + rolled[1]).reshape(16, 16, N)


def reduce_kernel(count, scalars, rows_ref, cols_ref, got_ref, out_ref):
    at = iota((16, N), 0)
    slot = M * (at // 8) + 8 * scalars[0] + at % 8
    lane = iota((16, N), 1)
    for part in (0, 1):
        sums = [jnp.zeros((16, N), F32)] * 4
        for p in range(count):
            value = got_ref[p, 0, part]
            low, wide = slot < rows_ref[p], lane < cols_ref[p]
            zero = jnp.zeros_like(value)
            below, above = jnp.where(low, value, zero), jnp.where(low, zero, value)
            for i, rows in enumerate((above, below)):
                sums[2 * i] += jnp.where(wide, zero, rows)
                sums[2 * i + 1] += jnp.where(wide, rows, zero)
        for strip in range(4):
            half, fold = strip % 2, strip // 2
            for side in (0, 1):
                out_ref[strip, 0, part, :, side * N : side * N + N] = sums[2 * fold + side][8 * half : 8 * half + 8]


def cut_kernel(rows_ref, cols_ref, starts_ref, *refs):
    blocks, out_ref = refs[:-1], refs[-1]
    strip, width = blocks[0].shape[-2:]
    height = strip * len(blocks)
    at = pl.program_id(0)
    held = iota((N, height), 1) % strip
    for i in range(len(blocks)):
        held += jnp.where(iota((N, height), 1) // strip == i, starts_ref[i], 0)
    rows = one_hot(paired_index((N, height), 0) + rows_ref[at], held)
    cols = one_hot(paired_index((width, N), 1) + cols_ref[at], iota((width, N), 0))
    for part in (0, 1):
        whole_part = jnp.concatenate([block[part, 0] for block in blocks], axis=0)
        out_ref[0, part] = dot(dot(rows, whole_part).astype(BF16), cols).astype(BF16)


def whole(shape):
    return pl.BlockSpec(shape, lambda *_: (0,) * len(shape))


SMEM = pl.BlockSpec(memory_space=pltpu.SMEM)
PARAMS = pltpu.CompilerParams(dimension_semantics=("arbitrary",), vmem_limit_bytes=48 << 20)
WAVE = (2, N, N)


def cut(blocks, starts, pos_rows, pos_cols):
    count = pos_rows.shape[0]
    return pl.pallas_call(
        cut_kernel,
        grid=(count,),
        in_specs=[SMEM] * 3 + [whole(blocks[0].shape)] * len(blocks),
        out_specs=pl.BlockSpec((1, 2, N, N), lambda i: (i, 0, 0, 0)),
        out_shape=jax.ShapeDtypeStruct((count, 2, N, N), BF16),
        compiler_params=PARAMS,
        name="cut",
    )(pos_rows, pos_cols, starts, *blocks)


def run_forward(mine, chunk, wave, prop, tabs, gain, inten=None):
    steps = chunk.shape[0]
    last = inten is not None
    extra = (inten,) if last else ()

    def body(*refs):
        forward_kernel(gain, last, steps, *refs)

    return pl.pallas_call(
        body,
        grid=(steps,),
        in_specs=[SMEM, pl.BlockSpec((1, 2, N, N), lambda i: (i, 0, 0, 0)), whole(WAVE), whole(WAVE)]
        + [whole((N, N))] * (4 + len(extra)),
        out_specs=[whole(WAVE), whole(WAVE)],
        out_shape=[jax.ShapeDtypeStruct(WAVE, F32)] * 2,
        compiler_params=PARAMS,
        name="forward",
    )(mine, chunk, wave, prop, *tabs, *extra)


def run_backward(scalars, chunk, ct, prop, tabs, kept, index, count, sent=None):
    steps = chunk.shape[0]

    def body(*refs):
        backward_kernel(steps, *refs)

    more = () if sent is None else (sent,)
    return pl.pallas_call(
        body,
        grid=(steps,),
        in_specs=[SMEM, pl.BlockSpec((1, 2, N, N), lambda i: (steps - 1 - i, 0, 0, 0)), whole(WAVE), whole(WAVE)]
        + [whole((N, N))] * 4
        + [whole(WAVE)]
        + [pl.BlockSpec(memory_space=pl.ANY)] * len(more),
        out_specs=[whole(WAVE), pl.BlockSpec((16, 1, 2, 16, N), lambda i: (0, index, 0, 0, 0))],
        out_shape=[jax.ShapeDtypeStruct(WAVE, F32), jax.ShapeDtypeStruct((16, count, 2, 16, N), F32)],
        scratch_shapes=[pltpu.VMEM(WAVE, F32)],
        input_output_aliases={9: 1} if more else {},
        compiler_params=PARAMS,
        name="backward",
    )(scalars, chunk, ct, prop, *tabs, kept, *more)


def run_reduce(piece, all_rows, all_cols, got):
    sources, count = got.shape[:2]

    def body(*refs):
        reduce_kernel(sources, *refs)

    return pl.pallas_call(
        body,
        grid=(count,),
        in_specs=[SMEM] * 3 + [pl.BlockSpec((sources, 1, 2, 16, N), lambda i: (0, i, 0, 0, 0))],
        out_specs=pl.BlockSpec((4, 1, 2, 8, 2 * N), lambda i: (0, i, 0, 0, 0)),
        out_shape=jax.ShapeDtypeStruct((4, count, 2, 8, 2 * N), F32),
        compiler_params=PARAMS,
        name="reduce",
    )(piece, all_rows, all_cols, got)


def from_neighbour(block, axis, distance):
    size = lax.axis_size(axis)
    return lax.ppermute(block, axis, [(i, (i + distance) % size) for i in range(size)])


def paired(x):
    for axis in (-2, -1):
        first, second = jnp.split(x, 2, axis=axis)
        x = jnp.concatenate([first, jnp.flip(second, axis=axis)], axis=axis)
    return x


def start_wave(probe_wave):
    at = np.arange(N)
    angle = math.pi / N * (at[:, None] + at[None, :])
    cos, sin = np.cos(angle).astype(np.float32), np.sin(angle).astype(np.float32)
    real, imag = probe_wave[0], probe_wave[1]
    return paired(jnp.stack([real * cos - imag * sin, real * sin + imag * cos]))


def on_device(probe_wave, object_field, pos_rows, pos_cols, intensity, prop_phase):
    row, tile = lax.axis_index("y"), lax.axis_index("x")
    mine = lax.axis_index("zc").astype(jnp.int32)
    chunks_count = lax.axis_size("y")
    strip, width = object_field.shape[2:]
    moves = (0, 1, 3, 2)
    blocks = [object_field] + [from_neighbour(object_field, "x", d) for d in moves[1:]]
    starts = jnp.stack([(tile - d) % 4 for d in moves]).astype(jnp.int32) * strip
    patches = cut(blocks, starts, pos_rows, pos_cols)
    patches = lax.all_to_all(patches, "y", 0, 0, tiled=True)
    chunks = [lax.all_gather(patches[i], "zc", axis=0) for i in range(chunks_count)]
    all_rows, all_cols = lax.all_gather(jnp.stack([pos_rows, pos_cols]), "x", axis=1, tiled=True)

    *tabs, gain = tables()
    tabs = [jnp.asarray(t) for t in tabs]
    prop = paired(jnp.stack([jnp.cos(prop_phase), jnp.sin(prop_phase)]) * (1.0 / gain))
    inten = paired(lax.dynamic_index_in_dim(intensity, row, 0, keepdims=False))
    wave = start_wave(probe_wave)
    mine_at = mine[None]
    scalars = jnp.stack([mine, pos_rows[row], pos_cols[row]])

    kept = []
    for i in range(chunks_count):
        last = i == chunks_count - 1
        wave, saved = run_forward(mine_at, chunks[i], wave, prop, tabs, gain, inten if last else None)
        kept.append(saved)
    sent = None
    for i in reversed(range(chunks_count)):
        wave, sent = run_backward(scalars, chunks[i], wave, prop, tabs, kept[i], i, chunks_count, sent)
    got = lax.all_to_all(sent, ("x", "y"), 0, 0, tiled=True)
    piece = (tile * 4 + row).astype(jnp.int32)[None]
    sums = run_reduce(piece, all_rows, all_cols, got).reshape(16, 2, 8, width)
    out = lax.all_to_all(sums, ("x", "y"), 0, 0, tiled=True)
    return jnp.transpose(out, (1, 0, 2, 3)).reshape(2, 1, strip, width)


def solution(mesh):
    devices = mesh.devices
    fine = Mesh(devices.reshape(4, devices.shape[0] // 4, devices.shape[1]), ("y", "zc", "x"))
    return jax.shard_map(
        on_device,
        mesh=fine,
        in_specs=(
            P(),
            P(None, ("y", "zc"), "x", None),
            P("x"),
            P("x"),
            P("x", None, None),
            P(),
        ),
        out_specs=P(None, ("y", "zc"), "x", None),
        check_vma=False,
    )
```

```python
import math

import jax
import jax.numpy as jnp
import ml_dtypes
import numpy as np
from jax import lax
from jax.experimental import pallas as pl
from jax.experimental.pallas import tpu as pltpu
from jax.sharding import Mesh, PartitionSpec as P

N = 256
M = N // 2
ROWS = 16
F32 = jnp.float32
BF16 = jnp.bfloat16


def tables():
    half = np.arange(M) + 0.5
    angles = 2.0 * math.pi / N * half[:, None] * half[None, :]
    packed, gain = [], []
    for values in (np.cos(angles) / 16.0, np.sin(angles) / 16.0):
        high = values.astype(ml_dtypes.bfloat16)
        low = (values - high.astype(np.float64)).astype(ml_dtypes.bfloat16)
        packed.append(np.block([[high, low], [high, low]]))
        both = high.astype(np.float64) + low.astype(np.float64)
        gain.append(4.0 * np.trace(both @ both) / M)
    at = np.arange(N)
    order = M * (at // ROWS % 2) + ROWS * (at // (2 * ROWS)) + at % ROWS
    lefts = [np.ascontiguousarray(table.T[order]) for table in packed]
    return *packed, *lefts, float(np.mean(gain)) ** 2


def split(x):
    high = x.astype(BF16)
    return high, (x - high.astype(F32)).astype(BF16)


def dot(a, b):
    return jnp.dot(a, b, preferred_element_type=F32)


def put_parts(ref, lead, at, value):
    high, low = split(value)
    ref[(*lead, pl.ds(at, ROWS), slice(0, M))] = high
    ref[(*lead, pl.ds(at, ROWS), slice(M, N))] = low


def put_folded(lhs_ref, part, at, values):
    for i, value in enumerate(values):
        put_parts(lhs_ref, (part, i % 2), M * (i // 2) + at, value)


def two_sided(lhs_ref, rhs_ref, tabs):
    cos_r, sin_r, cos_l, sin_l = tabs
    half = [[dot(lhs_ref[part, 0], cos_r), dot(lhs_ref[part, 1], sin_r)] for part in (0, 1)]
    out = []
    for part in (0, 1):
        for parity in (0, 1):
            for side in (0, 1):
                for at in range(0, M, ROWS):
                    rows = half[part][side][parity * M + at : parity * M + at + ROWS]
                    high, low = split(rows[:, :M] + rows[:, M:])
                    cols = slice(side * M, side * M + M)
                    rhs_ref[part, parity, at : at + ROWS, cols] = high
                    rhs_ref[part, parity, M + at : M + at + ROWS, cols] = low
        out.append([dot(cos_l, rhs_ref[part, 0]), dot(sin_l, rhs_ref[part, 1])])
    return out


def rows_of(out, part, at):
    got = []
    for parity in (0, 1):
        block = out[part][parity]
        rows = block[2 * at : 2 * at + ROWS] + block[2 * at + ROWS : 2 * at + 2 * ROWS]
        got += [rows[:, :M], rows[:, M:]]
    return got


def fold(x11, x12, x21, x22):
    d1, d2, s1, s2 = x11 - x21, x12 - x22, x11 + x21, x12 + x22
    return d1 - d2, d1 + d2, s1 - s2, s1 + s2


def unfold(uu, uv, vu, vv):
    p1, m1, p2, m2 = vv + uu, vv - uu, vu + uv, vu - uv
    return p1 + p2, m1 - m2, m1 + m2, p1 - p2


def spectrum_rows(out, at):
    ppr, pqr, qpr, qqr = rows_of(out, 0, at)
    ppi, pqi, qpi, qqi = rows_of(out, 1, at)
    ar, ai, br, bi = ppr - qqr, ppi - qqi, ppr + qqr, ppi + qqi
    er, ei, gr, gi = pqr + qpr, pqi + qpi, pqr - qpr, pqi - qpi
    return (ar + ei, br - gi, br + gi, ar - ei), (ai - er, bi + gr, bi - gr, ai + er)


def put_spectrum(lhs_ref, at, real, imag):
    yr11, yr12, yr21, yr22 = real
    yi11, yi12, yi21, yi22 = imag
    apr, api, amr, ami = yr11 + yr22, yi11 + yi22, yr11 - yr22, yi11 - yi22
    bpr, bpi, bmr, bmi = yr12 + yr21, yi12 + yi21, yr12 - yr21, yi12 - yi21
    put_folded(lhs_ref, 0, at, (apr + bpr, bmi - ami, -(ami + bmi), bpr - apr))
    put_folded(lhs_ref, 1, at, (api + bpi, amr - bmr, amr + bmr, bpi - api))


BLOCKS = range(0, M, ROWS)


def quads_at(ref, lead, at):
    return tuple(ref[(*lead, pl.ds(i * M + at, ROWS), slice(j * M, j * M + M))] for i in (0, 1) for j in (0, 1))


def put_quads(ref, part, at, values):
    for k, value in enumerate(values):
        ref[part, pl.ds(k // 2 * M + at, ROWS), slice(k % 2 * M, k % 2 * M + M)] = value


def times(ar, ai, br, bi):
    real = tuple(w * x - y * z for w, x, y, z in zip(ar, br, ai, bi))
    imag = tuple(w * z + y * x for w, x, y, z in zip(ar, br, ai, bi))
    return real, imag


def conj_times(ar, ai, br, bi):
    real = tuple(w * x + y * z for w, x, y, z in zip(ar, br, ai, bi))
    imag = tuple(w * z - y * x for w, x, y, z in zip(ar, br, ai, bi))
    return real, imag


def as_f32(values):
    return tuple(v.astype(F32) for v in values)


def load_pair(order, core, at, held, pair_ref):
    if len(held) == 2:
        pair_ref[core] = held[0][0, 0]
        pair_ref[1 - core] = held[1][0, 0]
        return
    for i in range(4):

        @pl.when(order[at] == i)
        def _():
            pair_ref[core] = held[i][...]
            pair_ref[1 - core] = held[4 + i][...]


def load_chunk(counts, refs, order, core, turn, at, pair_ref):
    first = 0
    for k, count in enumerate(counts):

        @pl.when(turn == k)
        def _(held=refs[first : first + count]):
            load_pair(order, core, at, held, pair_ref)

        first += count


def forward_kernel(gain, is_last, counts, stacks, order, scalars, *rest):
    held, (wave_ref, prop_ref, tabs_ref, *rest) = rest[: sum(counts)], rest[sum(counts) :]
    inten_ref, rest = (rest[0], rest[1:]) if is_last else (None, rest)
    out_ref, kept_ref, *stack_refs, pair_ref, lhs_ref, rhs_ref = rest
    step = pl.program_id(0)
    turn, at_z = step // 4, step % 4
    core = scalars[1]
    tabs = [tabs_ref[i] for i in range(4)]

    @pl.when(step == 0)
    def _():
        out_ref[...] = wave_ref[...]

    load_chunk(counts, held, order, core, turn, at_z, pair_ref)
    if stacks:
        stack_refs[0][0, 0] = pair_ref[core]
        stack_refs[1][0, 0] = pair_ref[1 - core]

    def one_slice(j, carry):
        @pl.when((at_z == scalars[0]) & (j == core))
        def _():
            kept_ref[turn] = out_ref[...]

        for at in BLOCKS:
            objr, obji = as_f32(quads_at(pair_ref, (j, 0), at)), as_f32(quads_at(pair_ref, (j, 1), at))
            mixed = times(quads_at(out_ref, (0,), at), quads_at(out_ref, (1,), at), objr, obji)
            for part in (0, 1):
                put_folded(lhs_ref, part, at, fold(*mixed[part]))
        spec = two_sided(lhs_ref, rhs_ref, tabs)
        for at in BLOCKS:
            real, imag = spectrum_rows(spec, at)
            put_spectrum(lhs_ref, at, *times(real, imag, quads_at(prop_ref, (0,), at), quads_at(prop_ref, (1,), at)))
        wave = two_sided(lhs_ref, rhs_ref, tabs)
        for at in BLOCKS:
            for part in (0, 1):
                put_quads(out_ref, part, at, unfold(*rows_of(wave, part, at)))
        return carry

    lax.fori_loop(0, 2, one_slice, 0)

    if is_last:

        @pl.when(step == pl.num_programs(0) - 1)
        def _():
            for at in BLOCKS:
                for part in (0, 1):
                    put_folded(lhs_ref, part, at, fold(*quads_at(out_ref, (part,), at)))
            spec = two_sided(lhs_ref, rhs_ref, tabs)
            for at in BLOCKS:
                real, imag = spectrum_rows(spec, at)
                measured = quads_at(inten_ref, (), at)
                scale = [(2.0 / gain) * (x * x + y * y - z) for x, y, z in zip(real, imag, measured)]
                put_spectrum(lhs_ref, at, [s * x for s, x in zip(scale, real)], [s * x for s, x in zip(scale, imag)])
            wave = two_sided(lhs_ref, rhs_ref, tabs)
            for at in BLOCKS:
                for part in (0, 1):
                    put_quads(out_ref, part, at, unfold(*rows_of(wave, part, at)))


def paired_index(shape, axis):
    at = lax.broadcasted_iota(jnp.int32, shape, axis)
    return jnp.where(at < M, at, N + M - 1 - at)


def one_hot(a, b):
    return jnp.where(a == b, 1.0, 0.0).astype(BF16)


def iota(shape, axis):
    return lax.broadcasted_iota(jnp.int32, shape, axis)


def backward_kernel(counts, order, scalars, *rest):
    chunks = len(counts)
    held, (ct_ref, prop_ref, tabs_ref, *rest) = rest[: sum(counts)], rest[sum(counts) :]
    kept_refs, rest = rest[:chunks], rest[chunks:]
    out_ref, sent_ref, grad_ref, mixed_ref, pair_ref, lhs_ref, rhs_ref = rest
    step = pl.program_id(0)
    chunk, at_z = chunks - 1 - step // 4, 3 - step % 4
    core = scalars[1]
    tabs = [tabs_ref[i] for i in range(4)]

    @pl.when(step == 0)
    def _():
        out_ref[...] = ct_ref[...]

    load_chunk(counts, held, order, core, chunk, at_z, pair_ref)

    def one_slice(turn, carry):
        j = 1 - turn
        for at in BLOCKS:
            for part in (0, 1):
                put_folded(lhs_ref, part, at, fold(*quads_at(out_ref, (part,), at)))
        spec = two_sided(lhs_ref, rhs_ref, tabs)
        for at in BLOCKS:
            prop = quads_at(prop_ref, (0,), at), quads_at(prop_ref, (1,), at)
            put_spectrum(lhs_ref, at, *conj_times(*prop, *spectrum_rows(spec, at)))
        wave = two_sided(lhs_ref, rhs_ref, tabs)
        for at in BLOCKS:
            mixed = [unfold(*rows_of(wave, part, at)) for part in (0, 1)]
            objr, obji = as_f32(quads_at(pair_ref, (j, 0), at)), as_f32(quads_at(pair_ref, (j, 1), at))
            back = conj_times(objr, obji, *mixed)
            for part in (0, 1):
                put_quads(mixed_ref, part, at, mixed[part])
                put_quads(out_ref, part, at, back[part])

        for k in range(chunks):

            @pl.when((chunk == k) & (at_z == scalars[0]) & (j == core))
            def _(kept_ref=kept_refs[k]):
                kr, ki, cr, ci = kept_ref[0, 0], kept_ref[0, 1], mixed_ref[0], mixed_ref[1]
                grad_ref[0] = kr * cr + ki * ci
                grad_ref[1] = kr * ci - ki * cr

        return carry

    lax.fori_loop(0, 2, one_slice, 0)

    @pl.when(at_z == 0)
    def _():
        at = iota((N, N), 0)
        slot = M * (at // 8 % 2) + 8 * (at // 16) + at % 8
        rows = one_hot((paired_index((N, N), 1) + scalars[2]) % N, slot)
        cols = one_hot((paired_index((N, N), 0) + scalars[3]) % N, iota((N, N), 1))
        for part in (0, 1):
            high, low = split(grad_ref[part])
            rolled = [dot(rows, dot(x, cols).astype(BF16)) for x in (high, low)]
            sent_ref[:, chunk, part] = (rolled[0] + rolled[1]).reshape(16, 16, N)


def reduce_kernel(count, scalars, tiles_ref, pos_ref, got_ref, out_ref):
    at = iota((16, N), 0)
    slot = M * (at // 8) + 8 * scalars[0] + at % 8
    lane = iota((16, N), 1)
    for part in (0, 1):
        sums = [jnp.zeros((16, N), F32)] * 4
        for p in range(count):
            value = got_ref[p, 0, part]
            held = tiles_ref[p // 4]
            low, wide = slot < pos_ref[held, 0, p % 4], lane < pos_ref[held, 1, p % 4]
            zero = jnp.zeros_like(value)
            below, above = jnp.where(low, value, zero), jnp.where(low, zero, value)
            for i, rows in enumerate((above, below)):
                sums[2 * i] += jnp.where(wide, zero, rows)
                sums[2 * i + 1] += jnp.where(wide, rows, zero)
        for strip in range(4):
            half, fold = strip % 2, strip // 2
            for side in (0, 1):
                out_ref[strip, 0, part, :, side * N : side * N + N] = sums[2 * fold + side][8 * half : 8 * half + 8]


def cut_kernel(rows_ref, cols_ref, starts_ref, *refs):
    blocks, out_ref = refs[:-1], refs[-1]
    strip, width = blocks[0].shape[-2:]
    height = strip * len(blocks)
    at = pl.program_id(0)
    held = iota((N, height), 1) % strip
    for i in range(len(blocks)):
        held += jnp.where(iota((N, height), 1) // strip == i, starts_ref[i], 0)
    rows = one_hot(paired_index((N, height), 0) + rows_ref[at], held)
    cols = one_hot(paired_index((width, N), 1) + cols_ref[at], iota((width, N), 0))
    for part in (0, 1):
        whole_part = jnp.concatenate([block[part, 0] for block in blocks], axis=0)
        out_ref[0, part] = dot(dot(rows, whole_part).astype(BF16), cols).astype(BF16)


def whole(shape):
    return pl.BlockSpec(shape, lambda *_: (0,) * len(shape))


SMEM = pl.BlockSpec(memory_space=pltpu.SMEM)
PARAMS = pltpu.CompilerParams(dimension_semantics=("arbitrary",), vmem_limit_bytes=24 << 20)
WAVE = (2, N, N)


def cost(chunks):
    return pl.CostEstimate(flops=chunks * 8 * 32 * N**3, bytes_accessed=chunks << 22, transcendentals=0)


def cut(blocks, starts, pos_rows, pos_cols):
    count = pos_rows.shape[0]
    return pl.pallas_call(
        cut_kernel,
        grid=(count,),
        in_specs=[SMEM] * 3 + [whole(blocks[0].shape)] * len(blocks),
        out_specs=pl.BlockSpec((1, 2, N, N), lambda i: (i, 0, 0, 0)),
        out_shape=jax.ShapeDtypeStruct((count, 2, N, N), BF16),
        compiler_params=PARAMS,
        name="cut",
    )(pos_rows, pos_cols, starts, *blocks)


def chunk_specs(chunks, reverse):
    specs, last = [], len(chunks) - 1
    for k, (blocks, at) in enumerate(chunks):
        if len(blocks) == 8:
            specs += [whole(WAVE)] * 8
            continue

        def block(i, *_, k=k, at=at):
            first = 4 * (last - k if reverse else k)
            inside = jnp.clip(i - first, 0, 3)
            return (3 - inside if reverse else inside, at, 0, 0, 0)

        specs += [pl.BlockSpec((1, 1, 2, N, N), block)] * 2
    return specs


def run_forward(order, scalars, chunks, wave, prop, tabs, gain, inten=None, stacks=False):
    counts = [len(blocks) for blocks, _ in chunks]
    last = inten is not None
    extra = (inten,) if last else ()

    def body(*refs):
        forward_kernel(gain, last, counts, stacks, *refs)

    kept = (len(chunks), *WAVE)
    stack = pl.BlockSpec((1, 1, 2, N, N), lambda i, *_: (i, 0, 0, 0, 0))
    return pl.pallas_call(
        body,
        grid_spec=pltpu.PrefetchScalarGridSpec(
            num_scalar_prefetch=2,
            grid=(4 * len(chunks),),
            in_specs=chunk_specs(chunks, False)
            + [whole(WAVE), whole(WAVE), whole((4, N, N))]
            + [whole((N, N))] * len(extra),
            out_specs=[whole(WAVE), whole(kept)] + [stack] * (2 * stacks),
            scratch_shapes=[pltpu.VMEM((2, 2, N, N), BF16)] * 3,
        ),
        out_shape=[jax.ShapeDtypeStruct(WAVE, F32), jax.ShapeDtypeStruct(kept, F32)]
        + [jax.ShapeDtypeStruct((4, 1, 2, N, N), BF16)] * (2 * stacks),
        compiler_params=PARAMS,
        cost_estimate=cost(len(chunks)),
        name="forward",
    )(order, scalars, *[x for blocks, _ in chunks for x in blocks], wave, prop, tabs, *extra)


def run_backward(order, scalars, chunks, ct, prop, tabs, kept):
    counts = [len(blocks) for blocks, _ in chunks]

    def body(*refs):
        backward_kernel(counts, *refs)

    sent = (16, len(chunks), 2, 16, N)
    return pl.pallas_call(
        body,
        grid_spec=pltpu.PrefetchScalarGridSpec(
            num_scalar_prefetch=2,
            grid=(4 * len(chunks),),
            in_specs=chunk_specs(chunks, True)
            + [whole(WAVE), whole(WAVE), whole((4, N, N))]
            + [pl.BlockSpec((1, *WAVE), lambda *_, at=at: (at, 0, 0, 0)) for _, at in kept],
            out_specs=[whole(WAVE), whole(sent)],
            scratch_shapes=[pltpu.VMEM(WAVE, F32)] * 2 + [pltpu.VMEM((2, 2, N, N), BF16)] * 3,
        ),
        out_shape=[jax.ShapeDtypeStruct(WAVE, F32), jax.ShapeDtypeStruct(sent, F32)],
        compiler_params=PARAMS,
        cost_estimate=cost(len(chunks)),
        name="backward",
    )(order, scalars, *[x for blocks, _ in chunks for x in blocks], ct, prop, tabs, *[x for x, _ in kept])


def run_reduce(piece, tiles, positions, got):
    sources, count = got.shape[:2]

    def body(*refs):
        reduce_kernel(sources, *refs)

    return pl.pallas_call(
        body,
        grid=(count,),
        in_specs=[SMEM] * 3 + [pl.BlockSpec((sources, 1, 2, 16, N), lambda i: (0, i, 0, 0, 0))],
        out_specs=pl.BlockSpec((4, 1, 2, 8, 2 * N), lambda i: (0, i, 0, 0, 0)),
        out_shape=jax.ShapeDtypeStruct((4, count, 2, 8, 2 * N), F32),
        compiler_params=PARAMS,
        name="reduce",
    )(piece, tiles, positions, got)


def from_neighbour(block, axis, distance):
    size = lax.axis_size(axis)
    return lax.ppermute(block, axis, [(i, (i + distance) % size) for i in range(size)])


def paired(x):
    for axis in (-2, -1):
        first, second = jnp.split(x, 2, axis=axis)
        x = jnp.concatenate([first, jnp.flip(second, axis=axis)], axis=axis)
    return x


def start_wave(probe_wave):
    at = np.arange(N)
    angle = math.pi / N * (at[:, None] + at[None, :])
    cos, sin = np.cos(angle).astype(np.float32), np.sin(angle).astype(np.float32)
    real, imag = probe_wave[0], probe_wave[1]
    return paired(jnp.stack([real * cos - imag * sin, real * sin + imag * cos]))


def around_of(at):
    return (at - jnp.arange(4, dtype=jnp.int32)) % 4


def ring_gather(block, z, core):
    size = lax.axis_size("z")
    below, above = from_neighbour(block, "z", 1), from_neighbour(block, "z", -1)
    route = [(2 * i + c, 2 * ((i + 1 - 2 * c) % size) + c) for i in range(size) for c in (0, 1)]
    far = lax.ppermute(jnp.where(core == 0, below, above), ("z", "core"), route)
    own = [block, below, far, above]
    return own + [from_neighbour(x, "core", 1) for x in own]


def on_device(probe_wave, object_field, pos_rows, pos_cols, intensity, prop_phase):
    row, tile, z, core = (lax.axis_index(name).astype(jnp.int32) for name in ("y", "x", "z", "core"))
    chunks_count = lax.axis_size("y")
    strip, width = object_field.shape[2:]
    moves = (0, 1, 3, 2)
    positions = jnp.stack([pos_rows, pos_cols])
    blocks = [object_field] + [from_neighbour(object_field, "x", d) for d in moves[1:]]
    positions = jnp.stack([positions] + [from_neighbour(positions, "x", d) for d in (1, 2, 3)])
    starts = jnp.stack([(tile - d) % 4 for d in moves]) * strip

    *tabs, gain = tables()
    tabs = jnp.asarray(np.stack(tabs))
    prop = paired(jnp.stack([jnp.cos(prop_phase), jnp.sin(prop_phase)]) * (1.0 / gain))
    inten = paired(lax.dynamic_index_in_dim(intensity, row, 0, keepdims=False))
    wave = start_wave(probe_wave)
    scalars = jnp.stack([z, core, pos_rows[row], pos_cols[row]])
    blocks, positions, prop, inten, wave, scalars = lax.optimization_barrier(
        (blocks, positions, prop, inten, wave, scalars)
    )

    patches = cut(blocks, starts, pos_rows, pos_cols)
    patches = lax.all_to_all(patches, "y", 0, 0, tiled=True)
    middle = lax.all_gather(patches[1:3], "z", axis=0)
    final = lax.all_gather(patches[3:], "z", axis=0)
    order = around_of(z)

    def forward(chunks, wave, **more):
        return run_forward(order, scalars, chunks, wave, prop, tabs, gain, **more)

    wave, kept0, *stacked = forward([(ring_gather(patches[0], z, core), 0)], wave, stacks=True)
    middle, wave = lax.optimization_barrier((middle, wave))
    middle = [middle, from_neighbour(middle, "core", 1)]
    wave, kept12 = forward([(middle, 0), (middle, 1)], wave)
    final, wave = lax.optimization_barrier((final, wave))
    final = [final, from_neighbour(final, "core", 1)]
    wave, kept3 = forward([(final, 0)], wave, inten=inten)

    def backward(chunks, wave, kept):
        return run_backward(order, scalars, chunks, wave, prop, tabs, kept)

    wave, sent23 = backward([(middle, 1), (final, 0)], wave, [(kept12, 1), (kept3, 0)])
    got23 = lax.all_to_all(sent23, ("x", "y"), 0, 0, tiled=True)
    wave, sent01 = backward([(stacked, 0), (middle, 0)], wave, [(kept0, 0), (kept12, 0)])
    got23, sent01 = lax.optimization_barrier((got23, sent01))
    got01 = lax.all_to_all(sent01, ("x", "y"), 0, 0, tiled=True)
    got = [got01, got23]
    piece = (tile * 4 + row)[None]
    sums = [run_reduce(piece, around_of(tile), positions, x) for x in got]
    sums = jnp.concatenate(sums, axis=1).reshape(16, 2, 8, width)
    out = lax.all_to_all(sums, ("x", "y"), 0, 0, tiled=True)
    return jnp.transpose(out, (1, 0, 2, 3)).reshape(2, 1, strip, width)


def solution(mesh):
    devices = mesh.devices
    fine = Mesh(devices.reshape(4, 4, 2, devices.shape[1]), ("y", "z", "core", "x"))
    cuts = ("y", "z", "core")
    return jax.shard_map(
        on_device,
        mesh=fine,
        in_specs=(
            P(),
            P(None, cuts, "x", None),
            P("x"),
            P("x"),
            P("x", None, None),
            P(),
        ),
        out_specs=P(None, cuts, "x", None),
        check_vma=False,
    )
```

```python
import math

import jax
import jax.numpy as jnp
import ml_dtypes
import numpy as np
from jax import lax
from jax.experimental import pallas as pl
from jax.experimental.pallas import tpu as pltpu
from jax.sharding import Mesh, PartitionSpec as P

N = 256
M = N // 2
ROWS = 16
F32 = jnp.float32
BF16 = jnp.bfloat16


def tables():
    half = np.arange(M) + 0.5
    angles = 2.0 * math.pi / N * half[:, None] * half[None, :]
    packed, gain = [], []
    for values in (np.cos(angles) / 16.0, np.sin(angles) / 16.0):
        high = values.astype(ml_dtypes.bfloat16)
        low = (values - high.astype(np.float64)).astype(ml_dtypes.bfloat16)
        packed.append(np.block([[high, low], [high, low]]))
        both = high.astype(np.float64) + low.astype(np.float64)
        gain.append(4.0 * np.trace(both @ both) / M)
    at = np.arange(N)
    order = M * (at // ROWS % 2) + ROWS * (at // (2 * ROWS)) + at % ROWS
    lefts = [np.ascontiguousarray(table.T[order]) for table in packed]
    return *packed, *lefts, float(np.mean(gain)) ** 2


def split(x):
    high = x.astype(BF16)
    return high, (x - high.astype(F32)).astype(BF16)


def dot(a, b):
    return jnp.dot(a, b, preferred_element_type=F32)


def put_parts(ref, lead, at, value):
    high, low = split(value)
    ref[(*lead, pl.ds(at, ROWS), slice(0, M))] = high
    ref[(*lead, pl.ds(at, ROWS), slice(M, N))] = low


def put_folded(lhs_ref, part, at, values):
    for i, value in enumerate(values):
        put_parts(lhs_ref, (part, i % 2), M * (i // 2) + at, value)


def two_sided(lhs_ref, rhs_ref, tabs):
    cos_r, sin_r, cos_l, sin_l = tabs
    half = [[dot(lhs_ref[part, 0], cos_r), dot(lhs_ref[part, 1], sin_r)] for part in (0, 1)]
    out = []
    for part in (0, 1):
        for parity in (0, 1):
            for side in (0, 1):
                for at in range(0, M, ROWS):
                    rows = half[part][side][parity * M + at : parity * M + at + ROWS]
                    high, low = split(rows[:, :M] + rows[:, M:])
                    cols = slice(side * M, side * M + M)
                    rhs_ref[part, parity, at : at + ROWS, cols] = high
                    rhs_ref[part, parity, M + at : M + at + ROWS, cols] = low
        out.append([dot(cos_l, rhs_ref[part, 0]), dot(sin_l, rhs_ref[part, 1])])
    return out


def rows_of(out, part, at):
    got = []
    for parity in (0, 1):
        block = out[part][parity]
        rows = block[2 * at : 2 * at + ROWS] + block[2 * at + ROWS : 2 * at + 2 * ROWS]
        got += [rows[:, :M], rows[:, M:]]
    return got


def fold(x11, x12, x21, x22):
    d1, d2, s1, s2 = x11 - x21, x12 - x22, x11 + x21, x12 + x22
    return d1 - d2, d1 + d2, s1 - s2, s1 + s2


def unfold(uu, uv, vu, vv):
    p1, m1, p2, m2 = vv + uu, vv - uu, vu + uv, vu - uv
    return p1 + p2, m1 - m2, m1 + m2, p1 - p2


def spectrum_rows(out, at):
    ppr, pqr, qpr, qqr = rows_of(out, 0, at)
    ppi, pqi, qpi, qqi = rows_of(out, 1, at)
    ar, ai, br, bi = ppr - qqr, ppi - qqi, ppr + qqr, ppi + qqi
    er, ei, gr, gi = pqr + qpr, pqi + qpi, pqr - qpr, pqi - qpi
    return (ar + ei, br - gi, br + gi, ar - ei), (ai - er, bi + gr, bi - gr, ai + er)


def put_spectrum(lhs_ref, at, real, imag):
    yr11, yr12, yr21, yr22 = real
    yi11, yi12, yi21, yi22 = imag
    apr, api, amr, ami = yr11 + yr22, yi11 + yi22, yr11 - yr22, yi11 - yi22
    bpr, bpi, bmr, bmi = yr12 + yr21, yi12 + yi21, yr12 - yr21, yi12 - yi21
    put_folded(lhs_ref, 0, at, (apr + bpr, bmi - ami, -(ami + bmi), bpr - apr))
    put_folded(lhs_ref, 1, at, (api + bpi, amr - bmr, amr + bmr, bpi - api))


BLOCKS = range(0, M, ROWS)


def quads_at(ref, lead, at):
    return tuple(ref[(*lead, pl.ds(i * M + at, ROWS), slice(j * M, j * M + M))] for i in (0, 1) for j in (0, 1))


def put_quads(ref, part, at, values):
    for k, value in enumerate(values):
        ref[part, pl.ds(k // 2 * M + at, ROWS), slice(k % 2 * M, k % 2 * M + M)] = value


def times(ar, ai, br, bi):
    real = tuple(w * x - y * z for w, x, y, z in zip(ar, br, ai, bi))
    imag = tuple(w * z + y * x for w, x, y, z in zip(ar, br, ai, bi))
    return real, imag


def conj_times(ar, ai, br, bi):
    real = tuple(w * x + y * z for w, x, y, z in zip(ar, br, ai, bi))
    imag = tuple(w * z - y * x for w, x, y, z in zip(ar, br, ai, bi))
    return real, imag


def as_f32(values):
    return tuple(v.astype(F32) for v in values)


def load_pair(order, core, at, held, pair_ref):
    if len(held) == 2:
        pair_ref[core] = held[0][0, 0]
        pair_ref[1 - core] = held[1][0, 0]
        return
    for i in range(4):

        @pl.when(order[at] == i)
        def _():
            pair_ref[core] = held[i][...]
            pair_ref[1 - core] = held[4 + i][...]


def load_chunk(counts, refs, order, core, turn, at, pair_ref):
    first = 0
    for k, count in enumerate(counts):

        @pl.when(turn == k)
        def _(held=refs[first : first + count]):
            load_pair(order, core, at, held, pair_ref)

        first += count


def forward_kernel(gain, is_last, counts, stacks, order, scalars, *rest):
    held, (wave_ref, prop_ref, tabs_ref, *rest) = rest[: sum(counts)], rest[sum(counts) :]
    inten_ref, rest = (rest[0], rest[1:]) if is_last else (None, rest)
    out_ref, kept_ref, *stack_refs, pair_ref, lhs_ref, rhs_ref = rest
    step = pl.program_id(0)
    turn, at_z = step // 4, step % 4
    core = scalars[1]
    tabs = [tabs_ref[i] for i in range(4)]

    @pl.when(step == 0)
    def _():
        out_ref[...] = wave_ref[...]

    load_chunk(counts, held, order, core, turn, at_z, pair_ref)
    if stacks:
        stack_refs[0][0, 0] = pair_ref[core]
        stack_refs[1][0, 0] = pair_ref[1 - core]

    def one_slice(j, carry):
        @pl.when((at_z == scalars[0]) & (j == core))
        def _():
            kept_ref[turn] = out_ref[...]

        for at in BLOCKS:
            objr, obji = as_f32(quads_at(pair_ref, (j, 0), at)), as_f32(quads_at(pair_ref, (j, 1), at))
            mixed = times(quads_at(out_ref, (0,), at), quads_at(out_ref, (1,), at), objr, obji)
            for part in (0, 1):
                put_folded(lhs_ref, part, at, fold(*mixed[part]))
        spec = two_sided(lhs_ref, rhs_ref, tabs)
        for at in BLOCKS:
            real, imag = spectrum_rows(spec, at)
            put_spectrum(lhs_ref, at, *times(real, imag, quads_at(prop_ref, (0,), at), quads_at(prop_ref, (1,), at)))
        wave = two_sided(lhs_ref, rhs_ref, tabs)
        for at in BLOCKS:
            for part in (0, 1):
                put_quads(out_ref, part, at, unfold(*rows_of(wave, part, at)))
        return carry

    lax.fori_loop(0, 2, one_slice, 0)

    if is_last:

        @pl.when(step == pl.num_programs(0) - 1)
        def _():
            for at in BLOCKS:
                for part in (0, 1):
                    put_folded(lhs_ref, part, at, fold(*quads_at(out_ref, (part,), at)))
            spec = two_sided(lhs_ref, rhs_ref, tabs)
            for at in BLOCKS:
                real, imag = spectrum_rows(spec, at)
                measured = quads_at(inten_ref, (), at)
                scale = [(2.0 / gain) * (x * x + y * y - z) for x, y, z in zip(real, imag, measured)]
                put_spectrum(lhs_ref, at, [s * x for s, x in zip(scale, real)], [s * x for s, x in zip(scale, imag)])
            wave = two_sided(lhs_ref, rhs_ref, tabs)
            for at in BLOCKS:
                for part in (0, 1):
                    put_quads(out_ref, part, at, unfold(*rows_of(wave, part, at)))


def paired_index(shape, axis):
    at = lax.broadcasted_iota(jnp.int32, shape, axis)
    return jnp.where(at < M, at, N + M - 1 - at)


def one_hot(a, b):
    return jnp.where(a == b, 1.0, 0.0).astype(BF16)


def iota(shape, axis):
    return lax.broadcasted_iota(jnp.int32, shape, axis)


def backward_kernel(counts, order, scalars, *rest):
    chunks = len(counts)
    held, (ct_ref, prop_ref, tabs_ref, *rest) = rest[: sum(counts)], rest[sum(counts) :]
    kept_refs, rest = rest[:chunks], rest[chunks:]
    out_ref, sent_ref, grad_ref, mixed_ref, pair_ref, lhs_ref, rhs_ref = rest
    step = pl.program_id(0)
    chunk, at_z = chunks - 1 - step // 4, 3 - step % 4
    core = scalars[1]
    tabs = [tabs_ref[i] for i in range(4)]

    @pl.when(step == 0)
    def _():
        out_ref[...] = ct_ref[...]

    load_chunk(counts, held, order, core, chunk, at_z, pair_ref)

    def one_slice(turn, carry):
        j = 1 - turn
        for at in BLOCKS:
            for part in (0, 1):
                put_folded(lhs_ref, part, at, fold(*quads_at(out_ref, (part,), at)))
        spec = two_sided(lhs_ref, rhs_ref, tabs)
        for at in BLOCKS:
            prop = quads_at(prop_ref, (0,), at), quads_at(prop_ref, (1,), at)
            put_spectrum(lhs_ref, at, *conj_times(*prop, *spectrum_rows(spec, at)))
        wave = two_sided(lhs_ref, rhs_ref, tabs)
        for at in BLOCKS:
            mixed = [unfold(*rows_of(wave, part, at)) for part in (0, 1)]
            objr, obji = as_f32(quads_at(pair_ref, (j, 0), at)), as_f32(quads_at(pair_ref, (j, 1), at))
            back = conj_times(objr, obji, *mixed)
            for part in (0, 1):
                put_quads(mixed_ref, part, at, mixed[part])
                put_quads(out_ref, part, at, back[part])

        for k in range(chunks):

            @pl.when((chunk == k) & (at_z == scalars[0]) & (j == core))
            def _(kept_ref=kept_refs[k]):
                kr, ki, cr, ci = kept_ref[0, 0], kept_ref[0, 1], mixed_ref[0], mixed_ref[1]
                grad_ref[0] = kr * cr + ki * ci
                grad_ref[1] = kr * ci - ki * cr

        return carry

    lax.fori_loop(0, 2, one_slice, 0)

    @pl.when(at_z == 0)
    def _():
        at = iota((N, N), 0)
        slot = M * (at // 8 % 2) + 8 * (at // 16) + at % 8
        rows = one_hot((paired_index((N, N), 1) + scalars[2]) % N, slot)
        cols = one_hot((paired_index((N, N), 0) + scalars[3]) % N, iota((N, N), 1))
        for part in (0, 1):
            high, low = split(grad_ref[part])
            rolled = [dot(rows, dot(x, cols).astype(BF16)) for x in (high, low)]
            sent_ref[:, chunk, part] = (rolled[0] + rolled[1]).reshape(16, 16, N)


def reduce_kernel(count, scalars, tiles_ref, pos_ref, got_ref, out_ref):
    at = iota((16, N), 0)
    slot = M * (at // 8) + 8 * scalars[0] + at % 8
    lane = iota((16, N), 1)
    for part in (0, 1):
        sums = [jnp.zeros((16, N), F32)] * 4
        for p in range(count):
            value = got_ref[p, 0, part]
            held = tiles_ref[p // 4]
            low, wide = slot < pos_ref[held, 0, p % 4], lane < pos_ref[held, 1, p % 4]
            zero = jnp.zeros_like(value)
            below, above = jnp.where(low, value, zero), jnp.where(low, zero, value)
            for i, rows in enumerate((above, below)):
                sums[2 * i] += jnp.where(wide, zero, rows)
                sums[2 * i + 1] += jnp.where(wide, rows, zero)
        for strip in range(4):
            half, fold = strip % 2, strip // 2
            for side in (0, 1):
                out_ref[strip, 0, part, :, side * N : side * N + N] = sums[2 * fold + side][8 * half : 8 * half + 8]


def cut_kernel(rows_ref, cols_ref, starts_ref, *refs):
    blocks, out_ref = refs[:-1], refs[-1]
    strip, width = blocks[0].shape[-2:]
    height = strip * len(blocks)
    at = pl.program_id(0)
    held = iota((N, height), 1) % strip
    for i in range(len(blocks)):
        held += jnp.where(iota((N, height), 1) // strip == i, starts_ref[i], 0)
    rows = one_hot(paired_index((N, height), 0) + rows_ref[at], held)
    cols = one_hot(paired_index((width, N), 1) + cols_ref[at], iota((width, N), 0))
    for part in (0, 1):
        whole_part = jnp.concatenate([block[part, 0] for block in blocks], axis=0)
        out_ref[0, part] = dot(dot(rows, whole_part).astype(BF16), cols).astype(BF16)


def whole(shape):
    return pl.BlockSpec(shape, lambda *_: (0,) * len(shape))


SMEM = pl.BlockSpec(memory_space=pltpu.SMEM)
PARAMS = pltpu.CompilerParams(dimension_semantics=("arbitrary",), vmem_limit_bytes=24 << 20)
WAVE = (2, N, N)


def cost(chunks):
    return pl.CostEstimate(flops=chunks * 8 * 32 * N**3, bytes_accessed=chunks << 22, transcendentals=0)


def cut(blocks, starts, pos_rows, pos_cols):
    count = pos_rows.shape[0]
    return pl.pallas_call(
        cut_kernel,
        grid=(count,),
        in_specs=[SMEM] * 3 + [whole(blocks[0].shape)] * len(blocks),
        out_specs=pl.BlockSpec((1, 2, N, N), lambda i: (i, 0, 0, 0)),
        out_shape=jax.ShapeDtypeStruct((count, 2, N, N), BF16),
        compiler_params=PARAMS,
        name="cut",
    )(pos_rows, pos_cols, starts, *blocks)


def chunk_specs(chunks, reverse):
    specs, last = [], len(chunks) - 1
    for k, (blocks, at) in enumerate(chunks):
        if len(blocks) == 8:
            specs += [whole(WAVE)] * 8
            continue

        def block(i, *_, k=k, at=at):
            first = 4 * (last - k if reverse else k)
            inside = jnp.clip(i - first, 0, 3)
            return (3 - inside if reverse else inside, at, 0, 0, 0)

        specs += [pl.BlockSpec((1, 1, 2, N, N), block)] * 2
    return specs


def run_forward(order, scalars, chunks, wave, prop, tabs, gain, inten=None, stacks=False):
    counts = [len(blocks) for blocks, _ in chunks]
    last = inten is not None
    extra = (inten,) if last else ()

    def body(*refs):
        forward_kernel(gain, last, counts, stacks, *refs)

    kept = (len(chunks), *WAVE)
    stack = pl.BlockSpec((1, 1, 2, N, N), lambda i, *_: (i, 0, 0, 0, 0))
    return pl.pallas_call(
        body,
        grid_spec=pltpu.PrefetchScalarGridSpec(
            num_scalar_prefetch=2,
            grid=(4 * len(chunks),),
            in_specs=chunk_specs(chunks, False)
            + [whole(WAVE), whole(WAVE), whole((4, N, N))]
            + [whole((N, N))] * len(extra),
            out_specs=[whole(WAVE), whole(kept)] + [stack] * (2 * stacks),
            scratch_shapes=[pltpu.VMEM((2, 2, N, N), BF16)] * 3,
        ),
        out_shape=[jax.ShapeDtypeStruct(WAVE, F32), jax.ShapeDtypeStruct(kept, F32)]
        + [jax.ShapeDtypeStruct((4, 1, 2, N, N), BF16)] * (2 * stacks),
        compiler_params=PARAMS,
        cost_estimate=cost(len(chunks)),
        name="forward",
    )(order, scalars, *in_hbm([x for blocks, _ in chunks for x in blocks]), wave, prop, tabs, *extra)


def run_backward(order, scalars, chunks, ct, prop, tabs, kept):
    counts = [len(blocks) for blocks, _ in chunks]

    def body(*refs):
        backward_kernel(counts, *refs)

    sent = (16, len(chunks), 2, 16, N)
    return pl.pallas_call(
        body,
        grid_spec=pltpu.PrefetchScalarGridSpec(
            num_scalar_prefetch=2,
            grid=(4 * len(chunks),),
            in_specs=chunk_specs(chunks, True)
            + [whole(WAVE), whole(WAVE), whole((4, N, N))]
            + [pl.BlockSpec((1, *WAVE), lambda *_, at=at: (at, 0, 0, 0)) for _, at in kept],
            out_specs=[whole(WAVE), whole(sent)],
            scratch_shapes=[pltpu.VMEM(WAVE, F32)] * 2 + [pltpu.VMEM((2, 2, N, N), BF16)] * 3,
        ),
        out_shape=[jax.ShapeDtypeStruct(WAVE, F32), jax.ShapeDtypeStruct(sent, F32)],
        compiler_params=PARAMS,
        cost_estimate=cost(len(chunks)),
        name="backward",
    )(order, scalars, *in_hbm([x for blocks, _ in chunks for x in blocks]), ct, prop, tabs, *[x for x, _ in kept])


def run_reduce(piece, tiles, positions, got):
    sources, count = got.shape[:2]

    def body(*refs):
        reduce_kernel(sources, *refs)

    return pl.pallas_call(
        body,
        grid=(count,),
        in_specs=[SMEM] * 3 + [pl.BlockSpec((sources, 1, 2, 16, N), lambda i: (0, i, 0, 0, 0))],
        out_specs=pl.BlockSpec((4, 1, 2, 8, 2 * N), lambda i: (0, i, 0, 0, 0)),
        out_shape=jax.ShapeDtypeStruct((4, count, 2, 8, 2 * N), F32),
        compiler_params=PARAMS,
        name="reduce",
    )(piece, tiles, positions, got)


def from_neighbour(block, axis, distance):
    size = lax.axis_size(axis)
    return lax.ppermute(block, axis, [(i, (i + distance) % size) for i in range(size)])


def paired(x):
    for axis in (-2, -1):
        first, second = jnp.split(x, 2, axis=axis)
        x = jnp.concatenate([first, jnp.flip(second, axis=axis)], axis=axis)
    return x


def start_wave(probe_wave):
    at = np.arange(N)
    angle = math.pi / N * (at[:, None] + at[None, :])
    cos, sin = np.cos(angle).astype(np.float32), np.sin(angle).astype(np.float32)
    real, imag = probe_wave[0], probe_wave[1]
    return paired(jnp.stack([real * cos - imag * sin, real * sin + imag * cos]))


def around_of(at):
    return (at - jnp.arange(4, dtype=jnp.int32)) % 4


def in_hbm(blocks):
    return [pltpu.with_memory_space_constraint(x, pltpu.HBM) for x in blocks]


def ring_gather(block):
    own = [block] + [from_neighbour(block, "z", d) for d in (1, 2, 3)]
    return own + [from_neighbour(x, "core", 1) for x in own]


def on_device(probe_wave, object_field, pos_rows, pos_cols, intensity, prop_phase):
    row, tile, z, core = (lax.axis_index(name).astype(jnp.int32) for name in ("y", "x", "z", "core"))
    chunks_count = lax.axis_size("y")
    strip, width = object_field.shape[2:]
    moves = (0, 1, 3, 2)
    positions = jnp.stack([pos_rows, pos_cols])
    blocks = [object_field] + [from_neighbour(object_field, "x", d) for d in moves[1:]]
    positions = jnp.stack([positions] + [from_neighbour(positions, "x", d) for d in (1, 2, 3)])
    starts = jnp.stack([(tile - d) % 4 for d in moves]) * strip

    *tabs, gain = tables()
    tabs = jnp.asarray(np.stack(tabs))
    prop = paired(jnp.stack([jnp.cos(prop_phase), jnp.sin(prop_phase)]) * (1.0 / gain))
    inten = paired(lax.dynamic_index_in_dim(intensity, row, 0, keepdims=False))
    wave = start_wave(probe_wave)
    scalars = jnp.stack([z, core, pos_rows[row], pos_cols[row]])
    patches = cut(blocks, starts, pos_rows, pos_cols)
    patches = lax.all_to_all(patches, "y", 0, 0, tiled=True)
    small = (positions, prop, inten, wave, scalars)
    patches, (positions, prop, inten, wave, scalars) = lax.optimization_barrier((patches, small))
    middle = lax.all_gather(patches[1:3], "z", axis=0)
    final = lax.all_gather(patches[3:], "z", axis=0)
    order = around_of(z)

    def forward(chunks, wave, **more):
        return run_forward(order, scalars, chunks, wave, prop, tabs, gain, **more)

    wave, kept0, *stacked = forward([(ring_gather(patches[0]), 0)], wave, stacks=True)
    middle, wave = lax.optimization_barrier((middle, wave))
    middle = [middle, from_neighbour(middle, "core", 1)]
    wave, kept12 = forward([(middle, 0), (middle, 1)], wave)
    final, wave = lax.optimization_barrier((final, wave))
    final = [final, from_neighbour(final, "core", 1)]
    wave, kept3 = forward([(final, 0)], wave, inten=inten)

    def backward(chunks, wave, kept):
        return run_backward(order, scalars, chunks, wave, prop, tabs, kept)

    wave, sent23 = backward([(middle, 1), (final, 0)], wave, [(kept12, 1), (kept3, 0)])
    got23 = lax.all_to_all(sent23, ("x", "y"), 0, 0, tiled=True)
    wave, sent01 = backward([(stacked, 0), (middle, 0)], wave, [(kept0, 0), (kept12, 0)])
    got23, sent01 = lax.optimization_barrier((got23, sent01))
    got01 = lax.all_to_all(sent01, ("x", "y"), 0, 0, tiled=True)
    got = [got01, got23]
    piece = (tile * 4 + row)[None]
    sums = [run_reduce(piece, around_of(tile), positions, x) for x in got]
    sums = jnp.concatenate(sums, axis=1).reshape(16, 2, 8, width)
    out = lax.all_to_all(sums, ("x", "y"), 0, 0, tiled=True)
    return jnp.transpose(out, (1, 0, 2, 3)).reshape(2, 1, strip, width)


def solution(mesh):
    devices = mesh.devices
    fine = Mesh(devices.reshape(4, 4, 2, devices.shape[1]), ("y", "z", "core", "x"))
    cuts = ("y", "z", "core")
    return jax.shard_map(
        on_device,
        mesh=fine,
        in_specs=(
            P(),
            P(None, cuts, "x", None),
            P("x"),
            P("x"),
            P("x", None, None),
            P(),
        ),
        out_specs=P(None, cuts, "x", None),
        check_vma=False,
    )
```

```python
import math

import jax
import jax.numpy as jnp
import ml_dtypes
import numpy as np
from jax import lax
from jax.experimental import pallas as pl
from jax.experimental.pallas import tpu as pltpu
from jax.sharding import Mesh, PartitionSpec as P

N = 256
M = N // 2
ROWS = 16
F32 = jnp.float32
BF16 = jnp.bfloat16


def tables():
    half = np.arange(M) + 0.5
    angles = 2.0 * math.pi / N * half[:, None] * half[None, :]
    packed, gain = [], []
    for values in (np.cos(angles) / 16.0, np.sin(angles) / 16.0):
        high = values.astype(ml_dtypes.bfloat16)
        low = (values - high.astype(np.float64)).astype(ml_dtypes.bfloat16)
        packed.append(np.block([[high, low], [high, low]]))
        both = high.astype(np.float64) + low.astype(np.float64)
        gain.append(4.0 * np.trace(both @ both) / M)
    at = np.arange(N)
    order = M * (at // ROWS % 2) + ROWS * (at // (2 * ROWS)) + at % ROWS
    lefts = [np.ascontiguousarray(table.T[order]) for table in packed]
    return *packed, *lefts, float(np.mean(gain)) ** 2


def split(x):
    high = x.astype(BF16)
    return high, (x - high.astype(F32)).astype(BF16)


def dot(a, b):
    return jnp.dot(a, b, preferred_element_type=F32)


def put_parts(ref, lead, at, value):
    high, low = split(value)
    ref[(*lead, pl.ds(at, ROWS), slice(0, M))] = high
    ref[(*lead, pl.ds(at, ROWS), slice(M, N))] = low


def put_folded(lhs_ref, part, at, values):
    for i, value in enumerate(values):
        put_parts(lhs_ref, (part, i % 2), M * (i // 2) + at, value)


def two_sided(lhs_ref, rhs_ref, tabs):
    cos_r, sin_r, cos_l, sin_l = tabs
    half = [[dot(lhs_ref[part, 0], cos_r), dot(lhs_ref[part, 1], sin_r)] for part in (0, 1)]
    out = []
    for part in (0, 1):
        for parity in (0, 1):
            for side in (0, 1):
                for at in range(0, M, ROWS):
                    rows = half[part][side][parity * M + at : parity * M + at + ROWS]
                    high, low = split(rows[:, :M] + rows[:, M:])
                    cols = slice(side * M, side * M + M)
                    rhs_ref[part, parity, at : at + ROWS, cols] = high
                    rhs_ref[part, parity, M + at : M + at + ROWS, cols] = low
        out.append([dot(cos_l, rhs_ref[part, 0]), dot(sin_l, rhs_ref[part, 1])])
    return out


def rows_of(out, part, at):
    got = []
    for parity in (0, 1):
        block = out[part][parity]
        rows = block[2 * at : 2 * at + ROWS] + block[2 * at + ROWS : 2 * at + 2 * ROWS]
        got += [rows[:, :M], rows[:, M:]]
    return got


def fold(x11, x12, x21, x22):
    d1, d2, s1, s2 = x11 - x21, x12 - x22, x11 + x21, x12 + x22
    return d1 - d2, d1 + d2, s1 - s2, s1 + s2


def unfold(uu, uv, vu, vv):
    p1, m1, p2, m2 = vv + uu, vv - uu, vu + uv, vu - uv
    return p1 + p2, m1 - m2, m1 + m2, p1 - p2


def spectrum_rows(out, at):
    ppr, pqr, qpr, qqr = rows_of(out, 0, at)
    ppi, pqi, qpi, qqi = rows_of(out, 1, at)
    ar, ai, br, bi = ppr - qqr, ppi - qqi, ppr + qqr, ppi + qqi
    er, ei, gr, gi = pqr + qpr, pqi + qpi, pqr - qpr, pqi - qpi
    return (ar + ei, br - gi, br + gi, ar - ei), (ai - er, bi + gr, bi - gr, ai + er)


def put_spectrum(lhs_ref, at, real, imag):
    yr11, yr12, yr21, yr22 = real
    yi11, yi12, yi21, yi22 = imag
    apr, api, amr, ami = yr11 + yr22, yi11 + yi22, yr11 - yr22, yi11 - yi22
    bpr, bpi, bmr, bmi = yr12 + yr21, yi12 + yi21, yr12 - yr21, yi12 - yi21
    put_folded(lhs_ref, 0, at, (apr + bpr, bmi - ami, -(ami + bmi), bpr - apr))
    put_folded(lhs_ref, 1, at, (api + bpi, amr - bmr, amr + bmr, bpi - api))


BLOCKS = range(0, M, ROWS)


def quads_at(ref, lead, at):
    return tuple(ref[(*lead, pl.ds(i * M + at, ROWS), slice(j * M, j * M + M))] for i in (0, 1) for j in (0, 1))


def put_quads(ref, part, at, values):
    for k, value in enumerate(values):
        ref[part, pl.ds(k // 2 * M + at, ROWS), slice(k % 2 * M, k % 2 * M + M)] = value


def times(ar, ai, br, bi):
    real = tuple(w * x - y * z for w, x, y, z in zip(ar, br, ai, bi))
    imag = tuple(w * z + y * x for w, x, y, z in zip(ar, br, ai, bi))
    return real, imag


def conj_times(ar, ai, br, bi):
    real = tuple(w * x + y * z for w, x, y, z in zip(ar, br, ai, bi))
    imag = tuple(w * z - y * x for w, x, y, z in zip(ar, br, ai, bi))
    return real, imag


def as_f32(values):
    return tuple(v.astype(F32) for v in values)


def load_pair(order, core, at, held, pair_ref):
    if len(held) == 1:
        pair_ref[...] = held[0][0]
        return
    if len(held) == 2:
        pair_ref[core] = held[0][0, 0]
        pair_ref[1 - core] = held[1][0, 0]
        return
    for i in range(4):

        @pl.when(order[at] == i)
        def _():
            pair_ref[core] = held[i][...]
            pair_ref[1 - core] = held[4 + i][...]


def load_chunk(counts, refs, order, core, turn, at, pair_ref):
    first = 0
    for k, count in enumerate(counts):

        @pl.when(turn == k)
        def _(held=refs[first : first + count]):
            load_pair(order, core, at, held, pair_ref)

        first += count


def forward_kernel(is_last, counts, stacks, order, scalars, *rest):
    held, (wave_ref, prop_ref, tabs_ref, *rest) = rest[: sum(counts)], rest[sum(counts) :]
    inten_ref, rest = (rest[0], rest[1:]) if is_last else (None, rest)
    out_ref, kept_ref, *stack_refs, pair_ref, lhs_ref, rhs_ref = rest
    step = pl.program_id(0)
    turn, at_z = step // 4, step % 4
    core = scalars[1]
    tabs = [tabs_ref[i] for i in range(4)]

    @pl.when(step == 0)
    def _():
        out_ref[...] = wave_ref[...]

    load_chunk(counts, held, order, core, turn, at_z, pair_ref)
    if stacks:
        stack_refs[0][0, 0] = pair_ref[core]
        stack_refs[1][0, 0] = pair_ref[1 - core]

    def one_slice(j, carry):
        @pl.when((at_z == scalars[0]) & (j == core))
        def _():
            kept_ref[turn] = out_ref[...]

        for at in BLOCKS:
            objr, obji = as_f32(quads_at(pair_ref, (j, 0), at)), as_f32(quads_at(pair_ref, (j, 1), at))
            mixed = times(quads_at(out_ref, (0,), at), quads_at(out_ref, (1,), at), objr, obji)
            for part in (0, 1):
                put_folded(lhs_ref, part, at, fold(*mixed[part]))
        spec = two_sided(lhs_ref, rhs_ref, tabs)
        for at in BLOCKS:
            prop = quads_at(prop_ref, (0,), at), quads_at(prop_ref, (1,), at)
            real, imag = times(*spectrum_rows(spec, at), *prop)
            if is_last:
                final = (step == pl.num_programs(0) - 1) & (j == 1)
                measured = quads_at(inten_ref, (), at)
                scale = [2.0 * (x * x + y * y - z) for x, y, z in zip(real, imag, measured)]
                slope = [[s * x for s, x in zip(scale, values)] for values in (real, imag)]
                back = conj_times(*prop, *slope)
                real, imag = ([jnp.where(final, b, a) for a, b in zip(*pair)] for pair in zip((real, imag), back))
            put_spectrum(lhs_ref, at, real, imag)
        wave = two_sided(lhs_ref, rhs_ref, tabs)
        for at in BLOCKS:
            for part in (0, 1):
                put_quads(out_ref, part, at, unfold(*rows_of(wave, part, at)))
        return carry

    lax.fori_loop(0, 2, one_slice, 0)


def paired_index(shape, axis):
    at = lax.broadcasted_iota(jnp.int32, shape, axis)
    return jnp.where(at < M, at, N + M - 1 - at)


def one_hot(a, b):
    return jnp.where(a == b, 1.0, 0.0).astype(BF16)


def iota(shape, axis):
    return lax.broadcasted_iota(jnp.int32, shape, axis)


def backward_kernel(from_end, counts, order, scalars, *rest):
    chunks = len(counts)
    held, (ct_ref, prop_ref, tabs_ref, *rest) = rest[: sum(counts)], rest[sum(counts) :]
    kept_refs, rest = rest[:chunks], rest[chunks:]
    out_ref, sent_ref, grad_ref, mixed_ref, pair_ref, lhs_ref, rhs_ref = rest
    step = pl.program_id(0)
    chunk, at_z = chunks - 1 - step // 4, 3 - step % 4
    core = scalars[1]
    tabs = [tabs_ref[i] for i in range(4)]

    @pl.when(step == 0)
    def _():
        out_ref[...] = ct_ref[...]

    load_chunk(counts, held, order, core, chunk, at_z, pair_ref)

    def one_slice(turn, carry):
        j = 1 - turn

        def put_back(at, mixed):
            objr, obji = as_f32(quads_at(pair_ref, (j, 0), at)), as_f32(quads_at(pair_ref, (j, 1), at))
            back = conj_times(objr, obji, *mixed)
            for part in (0, 1):
                put_quads(mixed_ref, part, at, mixed[part])
                put_quads(out_ref, part, at, back[part])

        def through():
            for at in BLOCKS:
                for part in (0, 1):
                    put_folded(lhs_ref, part, at, fold(*quads_at(out_ref, (part,), at)))
            spec = two_sided(lhs_ref, rhs_ref, tabs)
            for at in BLOCKS:
                prop = quads_at(prop_ref, (0,), at), quads_at(prop_ref, (1,), at)
                put_spectrum(lhs_ref, at, *conj_times(*prop, *spectrum_rows(spec, at)))
            wave = two_sided(lhs_ref, rhs_ref, tabs)
            for at in BLOCKS:
                put_back(at, [unfold(*rows_of(wave, part, at)) for part in (0, 1)])

        if from_end:
            at_end = (step == 0) & (turn == 0)
            pl.when(jnp.logical_not(at_end))(through)

            @pl.when(at_end)
            def _():
                for at in BLOCKS:
                    put_back(at, [quads_at(out_ref, (part,), at) for part in (0, 1)])

        else:
            through()

        for k in range(chunks):

            @pl.when((chunk == k) & (at_z == scalars[0]) & (j == core))
            def _(kept_ref=kept_refs[k]):
                kr, ki, cr, ci = kept_ref[0, 0], kept_ref[0, 1], mixed_ref[0], mixed_ref[1]
                grad_ref[0] = kr * cr + ki * ci
                grad_ref[1] = kr * ci - ki * cr

        return carry

    lax.fori_loop(0, 2, one_slice, 0)

    @pl.when(at_z == 0)
    def _():
        at = iota((N, N), 0)
        slot = M * (at // 8 % 2) + 8 * (at // 16) + at % 8
        rows = one_hot((paired_index((N, N), 1) + scalars[2]) % N, slot)
        cols = one_hot((paired_index((N, N), 0) + scalars[3]) % N, iota((N, N), 1))
        for part in (0, 1):
            high, low = split(grad_ref[part])
            rolled = [dot(rows, dot(x, cols).astype(BF16)) for x in (high, low)]
            sent_ref[:, chunk, part] = (rolled[0] + rolled[1]).reshape(16, 16, N)


def reduce_kernel(count, scalars, tiles_ref, pos_ref, got_ref, out_ref):
    at = iota((16, N), 0)
    slot = M * (at // 8) + 8 * scalars[0] + at % 8
    lane = iota((16, N), 1)
    for part in (0, 1):
        sums = [jnp.zeros((16, N), F32)] * 4
        for p in range(count):
            value = got_ref[p, 0, part]
            held = tiles_ref[p // 4]
            low, wide = slot < pos_ref[held, 0, p % 4], lane < pos_ref[held, 1, p % 4]
            zero = jnp.zeros_like(value)
            below, above = jnp.where(low, value, zero), jnp.where(low, zero, value)
            for i, rows in enumerate((above, below)):
                sums[2 * i] += jnp.where(wide, zero, rows)
                sums[2 * i + 1] += jnp.where(wide, rows, zero)
        for strip in range(4):
            half, fold = strip % 2, strip // 2
            for side in (0, 1):
                out_ref[strip, 0, part, :, side * N : side * N + N] = sums[2 * fold + side][8 * half : 8 * half + 8]


def cut_kernel(rows_ref, cols_ref, starts_ref, *refs):
    blocks, out_ref = refs[:-1], refs[-1]
    strip, width = blocks[0].shape[-2:]
    height = strip * len(blocks)
    at = pl.program_id(0)
    held = iota((N, height), 1) % strip
    for i in range(len(blocks)):
        held += jnp.where(iota((N, height), 1) // strip == i, starts_ref[i], 0)
    rows = one_hot(paired_index((N, height), 0) + rows_ref[at], held)
    cols = one_hot(paired_index((width, N), 1) + cols_ref[at], iota((width, N), 0))
    for part in (0, 1):
        whole_part = jnp.concatenate([block[part, 0] for block in blocks], axis=0)
        out_ref[0, part] = dot(dot(rows, whole_part).astype(BF16), cols).astype(BF16)


def whole(shape):
    return pl.BlockSpec(shape, lambda *_: (0,) * len(shape))


SMEM = pl.BlockSpec(memory_space=pltpu.SMEM)
PARAMS = pltpu.CompilerParams(dimension_semantics=("arbitrary",), vmem_limit_bytes=24 << 20)
WAVE = (2, N, N)


def cost(chunks):
    return pl.CostEstimate(flops=chunks * 8 * 32 * N**3, bytes_accessed=chunks << 22, transcendentals=0)


def cut(blocks, starts, pos_rows, pos_cols):
    count = pos_rows.shape[0]
    return pl.pallas_call(
        cut_kernel,
        grid=(count,),
        in_specs=[SMEM] * 3 + [whole(blocks[0].shape)] * len(blocks),
        out_specs=pl.BlockSpec((1, 2, N, N), lambda i: (i, 0, 0, 0)),
        out_shape=jax.ShapeDtypeStruct((count, 2, N, N), BF16),
        compiler_params=PARAMS,
        name="cut",
    )(pos_rows, pos_cols, starts, *blocks)


def chunk_specs(chunks, reverse):
    specs, last = [], len(chunks) - 1
    for k, (blocks, at) in enumerate(chunks):
        if len(blocks) == 8:
            specs += [whole(WAVE)] * 8
            continue

        def block(i, *_, k=k, at=at):
            first = 4 * (last - k if reverse else k)
            inside = jnp.clip(i - first, 0, 3)
            return (3 - inside if reverse else inside, at, 0, 0, 0)

        specs += [pl.BlockSpec((1, 3 - len(blocks), 2, N, N), block)] * len(blocks)
    return specs


def run_forward(order, scalars, chunks, wave, prop, tabs, inten=None, stacks=False):
    counts = [len(blocks) for blocks, _ in chunks]
    last = inten is not None
    extra = (inten,) if last else ()

    def body(*refs):
        forward_kernel(last, counts, stacks, *refs)

    kept = (len(chunks), *WAVE)
    stack = pl.BlockSpec((1, 1, 2, N, N), lambda i, *_: (i, 0, 0, 0, 0))
    return pl.pallas_call(
        body,
        grid_spec=pltpu.PrefetchScalarGridSpec(
            num_scalar_prefetch=2,
            grid=(4 * len(chunks),),
            in_specs=chunk_specs(chunks, False)
            + [whole(WAVE), whole(WAVE), whole((4, N, N))]
            + [whole((N, N))] * len(extra),
            out_specs=[whole(WAVE), whole(kept)] + [stack] * (2 * stacks),
            scratch_shapes=[pltpu.VMEM((2, 2, N, N), BF16)] * 3,
        ),
        out_shape=[jax.ShapeDtypeStruct(WAVE, F32), jax.ShapeDtypeStruct(kept, F32)]
        + [jax.ShapeDtypeStruct((4, 1, 2, N, N), BF16)] * (2 * stacks),
        compiler_params=PARAMS,
        cost_estimate=cost(len(chunks)),
        name="forward",
    )(order, scalars, *in_hbm([x for blocks, _ in chunks for x in blocks]), wave, prop, tabs, *extra)


def run_backward(order, scalars, chunks, ct, prop, tabs, kept, from_end=False):
    counts = [len(blocks) for blocks, _ in chunks]

    def body(*refs):
        backward_kernel(from_end, counts, *refs)

    sent = (16, len(chunks), 2, 16, N)
    return pl.pallas_call(
        body,
        grid_spec=pltpu.PrefetchScalarGridSpec(
            num_scalar_prefetch=2,
            grid=(4 * len(chunks),),
            in_specs=chunk_specs(chunks, True)
            + [whole(WAVE), whole(WAVE), whole((4, N, N))]
            + [pl.BlockSpec((1, *WAVE), lambda *_, at=at: (at, 0, 0, 0)) for _, at in kept],
            out_specs=[whole(WAVE), whole(sent)],
            scratch_shapes=[pltpu.VMEM(WAVE, F32)] * 2 + [pltpu.VMEM((2, 2, N, N), BF16)] * 3,
        ),
        out_shape=[jax.ShapeDtypeStruct(WAVE, F32), jax.ShapeDtypeStruct(sent, F32)],
        compiler_params=PARAMS,
        cost_estimate=cost(len(chunks)),
        name="backward",
    )(order, scalars, *in_hbm([x for blocks, _ in chunks for x in blocks]), ct, prop, tabs, *[x for x, _ in kept])


def run_reduce(piece, tiles, positions, got):
    sources, count = got.shape[:2]

    def body(*refs):
        reduce_kernel(sources, *refs)

    return pl.pallas_call(
        body,
        grid=(count,),
        in_specs=[SMEM] * 3 + [pl.BlockSpec((sources, 1, 2, 16, N), lambda i: (0, i, 0, 0, 0))],
        out_specs=pl.BlockSpec((4, 1, 2, 8, 2 * N), lambda i: (0, i, 0, 0, 0)),
        out_shape=jax.ShapeDtypeStruct((4, count, 2, 8, 2 * N), F32),
        compiler_params=PARAMS,
        name="reduce",
    )(piece, tiles, positions, got)


def from_neighbour(block, axis, distance):
    size = lax.axis_size(axis)
    return lax.ppermute(block, axis, [(i, (i + distance) % size) for i in range(size)])


def paired(x):
    for axis in (-2, -1):
        first, second = jnp.split(x, 2, axis=axis)
        x = jnp.concatenate([first, jnp.flip(second, axis=axis)], axis=axis)
    return x


def start_wave(probe_wave):
    at = np.arange(N)
    angle = math.pi / N * (at[:, None] + at[None, :])
    cos, sin = np.cos(angle).astype(np.float32), np.sin(angle).astype(np.float32)
    real, imag = probe_wave[0], probe_wave[1]
    return paired(jnp.stack([real * cos - imag * sin, real * sin + imag * cos]))


def around_of(at):
    return (at - jnp.arange(4, dtype=jnp.int32)) % 4


def in_hbm(blocks):
    return [pltpu.with_memory_space_constraint(x, pltpu.HBM) for x in blocks]


def ring_gather(block):
    own = [block] + [from_neighbour(block, "z", d) for d in (1, 2, 3)]
    return own + [from_neighbour(x, "core", 1) for x in own]


def on_device(probe_wave, object_field, pos_rows, pos_cols, intensity, prop_phase):
    row, tile, z, core = (lax.axis_index(name).astype(jnp.int32) for name in ("y", "x", "z", "core"))
    chunks_count = lax.axis_size("y")
    strip, width = object_field.shape[2:]
    moves = (0, 1, 3, 2)
    positions = jnp.stack([pos_rows, pos_cols])
    blocks = [object_field] + [from_neighbour(object_field, "x", d) for d in moves[1:]]
    starts = jnp.stack([(tile - d) % 4 for d in moves]) * strip

    *tabs, gain = tables()
    tabs = jnp.asarray(np.stack(tabs))
    prop = paired(jnp.stack([jnp.cos(prop_phase), jnp.sin(prop_phase)]) * (1.0 / gain))
    inten = paired(lax.dynamic_index_in_dim(intensity, row, 0, keepdims=False))
    wave = start_wave(probe_wave)
    scalars = jnp.stack([z, core, pos_rows[row], pos_cols[row]])
    patches = cut(blocks, starts, pos_rows, pos_cols)
    patches, positions = lax.optimization_barrier((patches, positions))
    positions = jnp.stack([positions] + [from_neighbour(positions, "x", d) for d in (1, 2, 3)])
    patches = lax.all_to_all(patches, "y", 0, 0, tiled=True)
    small = (positions, prop, inten, wave, scalars)
    patches, (positions, prop, inten, wave, scalars) = lax.optimization_barrier((patches, small))
    middle = lax.all_gather(patches[1:3], "z", axis=0)
    final = lax.all_gather(patches[3:], ("z", "core"), axis=0)
    order = around_of(z)

    def forward(chunks, wave, **more):
        return run_forward(order, scalars, chunks, wave, prop, tabs, **more)

    wave, kept0, *stacked = forward([(ring_gather(patches[0]), 0)], wave, stacks=True)
    middle, wave = lax.optimization_barrier((middle, wave))
    middle = [middle, from_neighbour(middle, "core", 1)]
    wave, kept12 = forward([(middle, 0), (middle, 1)], wave)
    final, wave = lax.optimization_barrier((final, wave))
    final = [final.reshape(4, 2, *WAVE)]
    wave, kept3 = forward([(final, 0)], wave, inten=inten)

    def backward(chunks, wave, kept, **more):
        return run_backward(order, scalars, chunks, wave, prop, tabs, kept, **more)

    wave, sent23 = backward([(middle, 1), (final, 0)], wave, [(kept12, 1), (kept3, 0)], from_end=True)
    got23 = lax.all_to_all(sent23, ("x", "y"), 0, 0, tiled=True)
    wave, sent01 = backward([(stacked, 0), (middle, 0)], wave, [(kept0, 0), (kept12, 0)])
    got23, sent01 = lax.optimization_barrier((got23, sent01))
    got01 = lax.all_to_all(sent01, ("x", "y"), 0, 0, tiled=True)
    got = [got01, got23]
    piece = (tile * 4 + row)[None]
    sums = [run_reduce(piece, around_of(tile), positions, x) for x in got]
    sums = jnp.concatenate(sums, axis=1).reshape(16, 2, 8, width)
    out = lax.all_to_all(sums, ("x", "y"), 0, 0, tiled=True)
    return jnp.transpose(out, (1, 0, 2, 3)).reshape(2, 1, strip, width)


def solution(mesh):
    devices = mesh.devices
    fine = Mesh(devices.reshape(4, 4, 2, devices.shape[1]), ("y", "z", "core", "x"))
    cuts = ("y", "z", "core")
    return jax.shard_map(
        on_device,
        mesh=fine,
        in_specs=(
            P(),
            P(None, cuts, "x", None),
            P("x"),
            P("x"),
            P("x", None, None),
            P(),
        ),
        out_specs=P(None, cuts, "x", None),
        check_vma=False,
    )
```

```python
import math

import jax
import jax.numpy as jnp
import ml_dtypes
import numpy as np
from jax import lax
from jax.experimental import pallas as pl
from jax.experimental.pallas import tpu as pltpu
from jax.sharding import Mesh, PartitionSpec as P

N = 256
M = N // 2
ROWS = 16
F32 = jnp.float32
BF16 = jnp.bfloat16


def tables():
    half = np.arange(M) + 0.5
    angles = 2.0 * math.pi / N * half[:, None] * half[None, :]
    packed, gain = [], []
    for values in (np.cos(angles) / 16.0, np.sin(angles) / 16.0):
        high = values.astype(ml_dtypes.bfloat16)
        low = (values - high.astype(np.float64)).astype(ml_dtypes.bfloat16)
        packed.append(np.block([[high, low], [high, low]]))
        both = high.astype(np.float64) + low.astype(np.float64)
        gain.append(4.0 * np.trace(both @ both) / M)
    at = np.arange(N)
    order = M * (at // ROWS % 2) + ROWS * (at // (2 * ROWS)) + at % ROWS
    lefts = [np.ascontiguousarray(table.T[order]) for table in packed]
    return *packed, *lefts, float(np.mean(gain)) ** 2


def split(x):
    high = x.astype(BF16)
    return high, (x - high.astype(F32)).astype(BF16)


def dot(a, b):
    return jnp.dot(a, b, preferred_element_type=F32)


def put_parts(ref, lead, at, value):
    high, low = split(value)
    ref[(*lead, pl.ds(at, ROWS), slice(0, M))] = high
    ref[(*lead, pl.ds(at, ROWS), slice(M, N))] = low


def put_folded(lhs_ref, part, at, values):
    for i, value in enumerate(values):
        put_parts(lhs_ref, (part, i % 2), M * (i // 2) + at, value)


def two_sided(lhs_ref, rhs_ref, tabs):
    cos_r, sin_r, cos_l, sin_l = tabs
    half = [[dot(lhs_ref[part, 0], cos_r), dot(lhs_ref[part, 1], sin_r)] for part in (0, 1)]
    out = []
    for part in (0, 1):
        for parity in (0, 1):
            for side in (0, 1):
                for at in range(0, M, ROWS):
                    rows = half[part][side][parity * M + at : parity * M + at + ROWS]
                    high, low = split(rows[:, :M] + rows[:, M:])
                    cols = slice(side * M, side * M + M)
                    rhs_ref[part, parity, at : at + ROWS, cols] = high
                    rhs_ref[part, parity, M + at : M + at + ROWS, cols] = low
        out.append([dot(cos_l, rhs_ref[part, 0]), dot(sin_l, rhs_ref[part, 1])])
    return out


def rows_of(out, part, at):
    got = []
    for parity in (0, 1):
        block = out[part][parity]
        rows = block[2 * at : 2 * at + ROWS] + block[2 * at + ROWS : 2 * at + 2 * ROWS]
        got += [rows[:, :M], rows[:, M:]]
    return got


def fold(x11, x12, x21, x22):
    d1, d2, s1, s2 = x11 - x21, x12 - x22, x11 + x21, x12 + x22
    return d1 - d2, d1 + d2, s1 - s2, s1 + s2


def unfold(uu, uv, vu, vv):
    p1, m1, p2, m2 = vv + uu, vv - uu, vu + uv, vu - uv
    return p1 + p2, m1 - m2, m1 + m2, p1 - p2


def spectrum_rows(out, at):
    ppr, pqr, qpr, qqr = rows_of(out, 0, at)
    ppi, pqi, qpi, qqi = rows_of(out, 1, at)
    ar, ai, br, bi = ppr - qqr, ppi - qqi, ppr + qqr, ppi + qqi
    er, ei, gr, gi = pqr + qpr, pqi + qpi, pqr - qpr, pqi - qpi
    return (ar + ei, br - gi, br + gi, ar - ei), (ai - er, bi + gr, bi - gr, ai + er)


def put_spectrum(lhs_ref, at, real, imag):
    yr11, yr12, yr21, yr22 = real
    yi11, yi12, yi21, yi22 = imag
    apr, api, amr, ami = yr11 + yr22, yi11 + yi22, yr11 - yr22, yi11 - yi22
    bpr, bpi, bmr, bmi = yr12 + yr21, yi12 + yi21, yr12 - yr21, yi12 - yi21
    put_folded(lhs_ref, 0, at, (apr + bpr, bmi - ami, -(ami + bmi), bpr - apr))
    put_folded(lhs_ref, 1, at, (api + bpi, amr - bmr, amr + bmr, bpi - api))


BLOCKS = range(0, M, ROWS)


def quads_at(ref, lead, at):
    return tuple(ref[(*lead, pl.ds(i * M + at, ROWS), slice(j * M, j * M + M))] for i in (0, 1) for j in (0, 1))


def put_quads(ref, part, at, values):
    for k, value in enumerate(values):
        ref[part, pl.ds(k // 2 * M + at, ROWS), slice(k % 2 * M, k % 2 * M + M)] = value


def times(ar, ai, br, bi):
    real = tuple(w * x - y * z for w, x, y, z in zip(ar, br, ai, bi))
    imag = tuple(w * z + y * x for w, x, y, z in zip(ar, br, ai, bi))
    return real, imag


def conj_times(ar, ai, br, bi):
    real = tuple(w * x + y * z for w, x, y, z in zip(ar, br, ai, bi))
    imag = tuple(w * z - y * x for w, x, y, z in zip(ar, br, ai, bi))
    return real, imag


def as_f32(values):
    return tuple(v.astype(F32) for v in values)


def load_pair(order, core, at, held, pair_ref):
    if len(held) == 1:
        pair_ref[...] = held[0][0]
        return
    if len(held) == 2:
        pair_ref[core] = held[0][0, 0]
        pair_ref[1 - core] = held[1][0, 0]
        return
    for i in range(4):

        @pl.when(order[at] == i)
        def _():
            pair_ref[core] = held[i][...]
            pair_ref[1 - core] = held[4 + i][...]


def load_chunk(counts, refs, order, core, turn, at, pair_ref):
    first = 0
    for k, count in enumerate(counts):

        @pl.when(turn == k)
        def _(held=refs[first : first + count]):
            load_pair(order, core, at, held, pair_ref)

        first += count


def forward_kernel(is_last, counts, stacks, order, scalars, *rest):
    held, (wave_ref, prop_ref, tabs_ref, *rest) = rest[: sum(counts)], rest[sum(counts) :]
    inten_ref, rest = (rest[0], rest[1:]) if is_last else (None, rest)
    out_ref, kept_ref, *stack_refs, pair_ref, lhs_ref, rhs_ref = rest
    step = pl.program_id(0)
    turn, at_z = step // 4, step % 4
    core = scalars[1]
    tabs = [tabs_ref[i] for i in range(4)]

    @pl.when(step == 0)
    def _():
        out_ref[...] = wave_ref[...]

    load_chunk(counts, held, order, core, turn, at_z, pair_ref)
    if stacks:
        stack_refs[0][0, 0] = pair_ref[core]
        stack_refs[1][0, 0] = pair_ref[1 - core]

    def one_slice(j, carry):
        @pl.when((at_z == scalars[0]) & (j == core))
        def _():
            kept_ref[turn] = out_ref[...]

        for at in BLOCKS:
            objr, obji = as_f32(quads_at(pair_ref, (j, 0), at)), as_f32(quads_at(pair_ref, (j, 1), at))
            mixed = times(quads_at(out_ref, (0,), at), quads_at(out_ref, (1,), at), objr, obji)
            for part in (0, 1):
                put_folded(lhs_ref, part, at, fold(*mixed[part]))
        spec = two_sided(lhs_ref, rhs_ref, tabs)
        for at in BLOCKS:
            prop = quads_at(prop_ref, (0,), at), quads_at(prop_ref, (1,), at)
            real, imag = times(*spectrum_rows(spec, at), *prop)
            if is_last:
                final = (step == pl.num_programs(0) - 1) & (j == 1)
                measured = quads_at(inten_ref, (), at)
                scale = [2.0 * (x * x + y * y - z) for x, y, z in zip(real, imag, measured)]
                slope = [[s * x for s, x in zip(scale, values)] for values in (real, imag)]
                back = conj_times(*prop, *slope)
                real, imag = ([jnp.where(final, b, a) for a, b in zip(*pair)] for pair in zip((real, imag), back))
            put_spectrum(lhs_ref, at, real, imag)
        wave = two_sided(lhs_ref, rhs_ref, tabs)
        for at in BLOCKS:
            for part in (0, 1):
                put_quads(out_ref, part, at, unfold(*rows_of(wave, part, at)))
        return carry

    lax.fori_loop(0, 2, one_slice, 0)


def paired_index(shape, axis):
    at = lax.broadcasted_iota(jnp.int32, shape, axis)
    return jnp.where(at < M, at, N + M - 1 - at)


def one_hot(a, b):
    return jnp.where(a == b, 1.0, 0.0).astype(BF16)


def iota(shape, axis):
    return lax.broadcasted_iota(jnp.int32, shape, axis)


def backward_kernel(from_end, counts, order, scalars, *rest):
    chunks = len(counts)
    held, (ct_ref, prop_ref, tabs_ref, *rest) = rest[: sum(counts)], rest[sum(counts) :]
    kept_refs, rest = rest[:chunks], rest[chunks:]
    out_ref, sent_ref, grad_ref, mixed_ref, pair_ref, lhs_ref, rhs_ref = rest
    step = pl.program_id(0)
    chunk, at_z = chunks - 1 - step // 4, 3 - step % 4
    core = scalars[1]
    tabs = [tabs_ref[i] for i in range(4)]

    @pl.when(step == 0)
    def _():
        out_ref[...] = ct_ref[...]

    load_chunk(counts, held, order, core, chunk, at_z, pair_ref)

    def one_slice(turn, carry):
        j = 1 - turn

        def put_back(at, mixed):
            objr, obji = as_f32(quads_at(pair_ref, (j, 0), at)), as_f32(quads_at(pair_ref, (j, 1), at))
            back = conj_times(objr, obji, *mixed)
            for part in (0, 1):
                put_quads(mixed_ref, part, at, mixed[part])
                put_quads(out_ref, part, at, back[part])

        def through():
            for at in BLOCKS:
                for part in (0, 1):
                    put_folded(lhs_ref, part, at, fold(*quads_at(out_ref, (part,), at)))
            spec = two_sided(lhs_ref, rhs_ref, tabs)
            for at in BLOCKS:
                prop = quads_at(prop_ref, (0,), at), quads_at(prop_ref, (1,), at)
                put_spectrum(lhs_ref, at, *conj_times(*prop, *spectrum_rows(spec, at)))
            wave = two_sided(lhs_ref, rhs_ref, tabs)
            for at in BLOCKS:
                put_back(at, [unfold(*rows_of(wave, part, at)) for part in (0, 1)])

        if from_end:
            at_end = (step == 0) & (turn == 0)
            pl.when(jnp.logical_not(at_end))(through)

            @pl.when(at_end)
            def _():
                for at in BLOCKS:
                    put_back(at, [quads_at(out_ref, (part,), at) for part in (0, 1)])

        else:
            through()

        for k in range(chunks):

            @pl.when((chunk == k) & (at_z == scalars[0]) & (j == core))
            def _(kept_ref=kept_refs[k]):
                kr, ki, cr, ci = kept_ref[0, 0], kept_ref[0, 1], mixed_ref[0], mixed_ref[1]
                grad_ref[0] = kr * cr + ki * ci
                grad_ref[1] = kr * ci - ki * cr

        return carry

    lax.fori_loop(0, 2, one_slice, 0)

    @pl.when(at_z == 0)
    def _():
        at = iota((N, N), 0)
        slot = M * (at // 8 % 2) + 8 * (at // 16) + at % 8
        rows = one_hot((paired_index((N, N), 1) + scalars[2]) % N, slot)
        cols = one_hot((paired_index((N, N), 0) + scalars[3]) % N, iota((N, N), 1))
        for part in (0, 1):
            high, low = split(grad_ref[part])
            rolled = [dot(rows, dot(x, cols).astype(BF16)) for x in (high, low)]
            sent_ref[:, chunk, part] = (rolled[0] + rolled[1]).reshape(16, 16, N)


def reduce_kernel(count, scalars, tiles_ref, pos_ref, got_ref, out_ref):
    at = iota((16, N), 0)
    slot = M * (at // 8) + 8 * scalars[0] + at % 8
    lane = iota((16, N), 1)
    for part in (0, 1):
        sums = [jnp.zeros((16, N), F32)] * 4
        for p in range(count):
            value = got_ref[p, 0, part]
            held = tiles_ref[p // 4]
            low, wide = slot < pos_ref[held, 0, p % 4], lane < pos_ref[held, 1, p % 4]
            zero = jnp.zeros_like(value)
            below, above = jnp.where(low, value, zero), jnp.where(low, zero, value)
            for i, rows in enumerate((above, below)):
                sums[2 * i] += jnp.where(wide, zero, rows)
                sums[2 * i + 1] += jnp.where(wide, rows, zero)
        for strip in range(4):
            half, fold = strip % 2, strip // 2
            for side in (0, 1):
                out_ref[strip, 0, part, :, side * N : side * N + N] = sums[2 * fold + side][8 * half : 8 * half + 8]


def cut_kernel(rows_ref, cols_ref, starts_ref, *refs):
    blocks, out_ref = refs[:-1], refs[-1]
    strip, width = blocks[0].shape[-2:]
    height = strip * len(blocks)
    at = pl.program_id(0)
    held = iota((N, height), 1) % strip
    for i in range(len(blocks)):
        held += jnp.where(iota((N, height), 1) // strip == i, starts_ref[i], 0)
    rows = one_hot(paired_index((N, height), 0) + rows_ref[at], held)
    cols = one_hot(paired_index((width, N), 1) + cols_ref[at], iota((width, N), 0))
    for part in (0, 1):
        whole_part = jnp.concatenate([block[part, 0] for block in blocks], axis=0)
        out_ref[0, part] = dot(dot(rows, whole_part).astype(BF16), cols).astype(BF16)


def whole(shape):
    return pl.BlockSpec(shape, lambda *_: (0,) * len(shape))


SMEM = pl.BlockSpec(memory_space=pltpu.SMEM)
PARAMS = pltpu.CompilerParams(dimension_semantics=("arbitrary",), vmem_limit_bytes=24 << 20)
WAVE = (2, N, N)


def cost(chunks):
    return pl.CostEstimate(flops=chunks * 8 * 32 * N**3, bytes_accessed=chunks << 22, transcendentals=0)


def cut(blocks, starts, pos_rows, pos_cols):
    count = pos_rows.shape[0]
    return pl.pallas_call(
        cut_kernel,
        grid=(count,),
        in_specs=[SMEM] * 3 + [whole(blocks[0].shape)] * len(blocks),
        out_specs=pl.BlockSpec((1, 2, N, N), lambda i: (i, 0, 0, 0)),
        out_shape=jax.ShapeDtypeStruct((count, 2, N, N), BF16),
        compiler_params=PARAMS,
        name="cut",
    )(pos_rows, pos_cols, starts, *blocks)


def chunk_specs(chunks, reverse):
    specs, last = [], len(chunks) - 1
    for k, (blocks, at) in enumerate(chunks):
        if len(blocks) == 8:
            specs += [whole(WAVE)] * 8
            continue

        def block(i, *_, k=k, at=at):
            first = 4 * (last - k if reverse else k)
            inside = jnp.clip(i - first, 0, 3)
            return (3 - inside if reverse else inside, at, 0, 0, 0)

        specs += [pl.BlockSpec((1, 3 - len(blocks), 2, N, N), block)] * len(blocks)
    return specs


def run_forward(order, scalars, chunks, wave, prop, tabs, inten=None, stacks=False):
    counts = [len(blocks) for blocks, _ in chunks]
    last = inten is not None
    extra = (inten,) if last else ()

    def body(*refs):
        forward_kernel(last, counts, stacks, *refs)

    kept = (len(chunks), *WAVE)
    stack = pl.BlockSpec((1, 1, 2, N, N), lambda i, *_: (i, 0, 0, 0, 0))
    return pl.pallas_call(
        body,
        grid_spec=pltpu.PrefetchScalarGridSpec(
            num_scalar_prefetch=2,
            grid=(4 * len(chunks),),
            in_specs=chunk_specs(chunks, False)
            + [whole(WAVE), whole(WAVE), whole((4, N, N))]
            + [whole((N, N))] * len(extra),
            out_specs=[whole(WAVE), whole(kept)] + [stack] * (2 * stacks),
            scratch_shapes=[pltpu.VMEM((2, 2, N, N), BF16)] * 3,
        ),
        out_shape=[jax.ShapeDtypeStruct(WAVE, F32), jax.ShapeDtypeStruct(kept, F32)]
        + [pltpu.HBM((4, 1, 2, N, N), BF16)] * (2 * stacks),
        compiler_params=PARAMS,
        cost_estimate=cost(len(chunks)),
        name="forward",
    )(order, scalars, *in_hbm([x for blocks, _ in chunks for x in blocks]), wave, prop, tabs, *extra)


def run_backward(order, scalars, chunks, ct, prop, tabs, kept, from_end=False):
    counts = [len(blocks) for blocks, _ in chunks]

    def body(*refs):
        backward_kernel(from_end, counts, *refs)

    sent = (16, len(chunks), 2, 16, N)
    return pl.pallas_call(
        body,
        grid_spec=pltpu.PrefetchScalarGridSpec(
            num_scalar_prefetch=2,
            grid=(4 * len(chunks),),
            in_specs=chunk_specs(chunks, True)
            + [whole(WAVE), whole(WAVE), whole((4, N, N))]
            + [pl.BlockSpec((1, *WAVE), lambda *_, at=at: (at, 0, 0, 0)) for _, at in kept],
            out_specs=[whole(WAVE), whole(sent)],
            scratch_shapes=[pltpu.VMEM(WAVE, F32)] * 2 + [pltpu.VMEM((2, 2, N, N), BF16)] * 3,
        ),
        out_shape=[jax.ShapeDtypeStruct(WAVE, F32), jax.ShapeDtypeStruct(sent, F32)],
        compiler_params=PARAMS,
        cost_estimate=cost(len(chunks)),
        name="backward",
    )(order, scalars, *in_hbm([x for blocks, _ in chunks for x in blocks]), ct, prop, tabs, *[x for x, _ in kept])


def run_reduce(piece, tiles, positions, got):
    sources, count = got.shape[:2]

    def body(*refs):
        reduce_kernel(sources, *refs)

    return pl.pallas_call(
        body,
        grid=(count,),
        in_specs=[SMEM] * 3 + [pl.BlockSpec((sources, 1, 2, 16, N), lambda i: (0, i, 0, 0, 0))],
        out_specs=pl.BlockSpec((4, 1, 2, 8, 2 * N), lambda i: (0, i, 0, 0, 0)),
        out_shape=jax.ShapeDtypeStruct((4, count, 2, 8, 2 * N), F32),
        compiler_params=PARAMS,
        name="reduce",
    )(piece, tiles, positions, got)


def from_neighbour(block, axis, distance):
    size = lax.axis_size(axis)
    return lax.ppermute(block, axis, [(i, (i + distance) % size) for i in range(size)])


def paired(x):
    for axis in (-2, -1):
        first, second = jnp.split(x, 2, axis=axis)
        x = jnp.concatenate([first, jnp.flip(second, axis=axis)], axis=axis)
    return x


def start_wave(probe_wave):
    at = np.arange(N)
    angle = math.pi / N * (at[:, None] + at[None, :])
    cos, sin = np.cos(angle).astype(np.float32), np.sin(angle).astype(np.float32)
    real, imag = probe_wave[0], probe_wave[1]
    return paired(jnp.stack([real * cos - imag * sin, real * sin + imag * cos]))


def around_of(at):
    return (at - jnp.arange(4, dtype=jnp.int32)) % 4


def in_hbm(blocks):
    return [pltpu.with_memory_space_constraint(x, pltpu.HBM) for x in blocks]


def ring_gather(block):
    own = [block] + [from_neighbour(block, "z", d) for d in (1, 2, 3)]
    return own + [from_neighbour(x, "core", 1) for x in own]


def on_device(probe_wave, object_field, pos_rows, pos_cols, intensity, prop_phase):
    row, tile, z, core = (lax.axis_index(name).astype(jnp.int32) for name in ("y", "x", "z", "core"))
    chunks_count = lax.axis_size("y")
    strip, width = object_field.shape[2:]
    moves = (0, 1, 3, 2)
    positions = jnp.stack([pos_rows, pos_cols])
    blocks = [object_field] + [from_neighbour(object_field, "x", d) for d in moves[1:]]
    starts = jnp.stack([(tile - d) % 4 for d in moves]) * strip

    *tabs, gain = tables()
    tabs = jnp.asarray(np.stack(tabs))
    prop = paired(jnp.stack([jnp.cos(prop_phase), jnp.sin(prop_phase)]) * (1.0 / gain))
    inten = paired(lax.dynamic_index_in_dim(intensity, row, 0, keepdims=False))
    wave = start_wave(probe_wave)
    scalars = jnp.stack([z, core, pos_rows[row], pos_cols[row]])
    patches = cut(blocks, starts, pos_rows, pos_cols)
    patches, positions = lax.optimization_barrier((patches, positions))
    positions = jnp.stack([positions] + [from_neighbour(positions, "x", d) for d in (1, 2, 3)])
    patches = lax.all_to_all(patches, "y", 0, 0, tiled=True)
    small = (positions, prop, inten, wave, scalars)
    patches, (positions, prop, inten, wave, scalars) = lax.optimization_barrier((patches, small))
    middle = lax.all_gather(patches[1:3], "z", axis=0)
    final = lax.all_gather(patches[3:], ("z", "core"), axis=0)
    order = around_of(z)

    def forward(chunks, wave, **more):
        return run_forward(order, scalars, chunks, wave, prop, tabs, **more)

    wave, kept0, *stacked = forward([(ring_gather(patches[0]), 0)], wave, stacks=True)
    middle, wave = lax.optimization_barrier((middle, wave))
    middle = [middle, from_neighbour(middle, "core", 1)]
    wave, kept12 = forward([(middle, 0), (middle, 1)], wave)
    final, wave = lax.optimization_barrier((final, wave))
    final = [final.reshape(4, 2, *WAVE)]
    wave, kept3 = forward([(final, 0)], wave, inten=inten)

    def backward(chunks, wave, kept, **more):
        return run_backward(order, scalars, chunks, wave, prop, tabs, kept, **more)

    wave, sent23 = backward([(middle, 1), (final, 0)], wave, [(kept12, 1), (kept3, 0)], from_end=True)
    got23 = lax.all_to_all(sent23, ("x", "y"), 0, 0, tiled=True)
    wave, sent01 = backward([(stacked, 0), (middle, 0)], wave, [(kept0, 0), (kept12, 0)])
    got23, sent01 = lax.optimization_barrier((got23, sent01))
    got01 = lax.all_to_all(sent01, ("x", "y"), 0, 0, tiled=True)
    got = [got01, got23]
    piece = (tile * 4 + row)[None]
    sums = [run_reduce(piece, around_of(tile), positions, x) for x in got]
    sums = jnp.concatenate(sums, axis=1).reshape(16, 2, 8, width)
    out = lax.all_to_all(sums, ("x", "y"), 0, 0, tiled=True)
    return jnp.transpose(out, (1, 0, 2, 3)).reshape(2, 1, strip, width)


def solution(mesh):
    devices = mesh.devices
    fine = Mesh(devices.reshape(4, 4, 2, devices.shape[1]), ("y", "z", "core", "x"))
    cuts = ("y", "z", "core")
    return jax.shard_map(
        on_device,
        mesh=fine,
        in_specs=(
            P(),
            P(None, cuts, "x", None),
            P("x"),
            P("x"),
            P("x", None, None),
            P(),
        ),
        out_specs=P(None, cuts, "x", None),
        check_vma=False,
    )
```

```python
import math

import jax
import jax.numpy as jnp
import ml_dtypes
import numpy as np
from jax import lax
from jax.experimental import pallas as pl
from jax.experimental.pallas import tpu as pltpu
from jax.sharding import Mesh, PartitionSpec as P

N = 256
M = N // 2
ROWS = 16
F32 = jnp.float32
BF16 = jnp.bfloat16


def tables():
    half = np.arange(M) + 0.5
    angles = 2.0 * math.pi / N * half[:, None] * half[None, :]
    packed, gain = [], []
    for values in (np.cos(angles) / 16.0, np.sin(angles) / 16.0):
        high = values.astype(ml_dtypes.bfloat16)
        low = (values - high.astype(np.float64)).astype(ml_dtypes.bfloat16)
        packed.append(np.block([[high, low], [high, low]]))
        both = high.astype(np.float64) + low.astype(np.float64)
        gain.append(4.0 * np.trace(both @ both) / M)
    at = np.arange(N)
    order = M * (at // ROWS % 2) + ROWS * (at // (2 * ROWS)) + at % ROWS
    lefts = [np.ascontiguousarray(table.T[order]) for table in packed]
    return *packed, *lefts, float(np.mean(gain)) ** 2


def split(x):
    high = x.astype(BF16)
    return high, (x - high.astype(F32)).astype(BF16)


def dot(a, b):
    return jnp.dot(a, b, preferred_element_type=F32)


def put_parts(ref, lead, at, value):
    high, low = split(value)
    ref[(*lead, pl.ds(at, ROWS), slice(0, M))] = high
    ref[(*lead, pl.ds(at, ROWS), slice(M, N))] = low


def put_folded(lhs_ref, part, at, values):
    for i, value in enumerate(values):
        put_parts(lhs_ref, (part, i % 2), M * (i // 2) + at, value)


def two_sided(lhs_ref, rhs_ref, tabs):
    cos_r, sin_r, cos_l, sin_l = tabs
    half = [[dot(lhs_ref[part, 0], cos_r), dot(lhs_ref[part, 1], sin_r)] for part in (0, 1)]
    out = []
    for part in (0, 1):
        for parity in (0, 1):
            for side in (0, 1):
                for at in range(0, M, ROWS):
                    rows = half[part][side][parity * M + at : parity * M + at + ROWS]
                    high, low = split(rows[:, :M] + rows[:, M:])
                    cols = slice(side * M, side * M + M)
                    rhs_ref[part, parity, at : at + ROWS, cols] = high
                    rhs_ref[part, parity, M + at : M + at + ROWS, cols] = low
        out.append([dot(cos_l, rhs_ref[part, 0]), dot(sin_l, rhs_ref[part, 1])])
    return out


def rows_of(out, part, at):
    got = []
    for parity in (0, 1):
        block = out[part][parity]
        rows = block[2 * at : 2 * at + ROWS] + block[2 * at + ROWS : 2 * at + 2 * ROWS]
        got += [rows[:, :M], rows[:, M:]]
    return got


def fold(x11, x12, x21, x22):
    d1, d2, s1, s2 = x11 - x21, x12 - x22, x11 + x21, x12 + x22
    return d1 - d2, d1 + d2, s1 - s2, s1 + s2


def unfold(uu, uv, vu, vv):
    p1, m1, p2, m2 = vv + uu, vv - uu, vu + uv, vu - uv
    return p1 + p2, m1 - m2, m1 + m2, p1 - p2


def spectrum_rows(out, at):
    ppr, pqr, qpr, qqr = rows_of(out, 0, at)
    ppi, pqi, qpi, qqi = rows_of(out, 1, at)
    ar, ai, br, bi = ppr - qqr, ppi - qqi, ppr + qqr, ppi + qqi
    er, ei, gr, gi = pqr + qpr, pqi + qpi, pqr - qpr, pqi - qpi
    return (ar + ei, br - gi, br + gi, ar - ei), (ai - er, bi + gr, bi - gr, ai + er)


def put_spectrum(lhs_ref, at, real, imag):
    yr11, yr12, yr21, yr22 = real
    yi11, yi12, yi21, yi22 = imag
    apr, api, amr, ami = yr11 + yr22, yi11 + yi22, yr11 - yr22, yi11 - yi22
    bpr, bpi, bmr, bmi = yr12 + yr21, yi12 + yi21, yr12 - yr21, yi12 - yi21
    put_folded(lhs_ref, 0, at, (apr + bpr, bmi - ami, -(ami + bmi), bpr - apr))
    put_folded(lhs_ref, 1, at, (api + bpi, amr - bmr, amr + bmr, bpi - api))


BLOCKS = range(0, M, ROWS)


def quads_at(ref, lead, at):
    return tuple(ref[(*lead, pl.ds(i * M + at, ROWS), slice(j * M, j * M + M))] for i in (0, 1) for j in (0, 1))


def put_quads(ref, part, at, values):
    for k, value in enumerate(values):
        ref[part, pl.ds(k // 2 * M + at, ROWS), slice(k % 2 * M, k % 2 * M + M)] = value


def times(ar, ai, br, bi):
    real = tuple(w * x - y * z for w, x, y, z in zip(ar, br, ai, bi))
    imag = tuple(w * z + y * x for w, x, y, z in zip(ar, br, ai, bi))
    return real, imag


def conj_times(ar, ai, br, bi):
    real = tuple(w * x + y * z for w, x, y, z in zip(ar, br, ai, bi))
    imag = tuple(w * z - y * x for w, x, y, z in zip(ar, br, ai, bi))
    return real, imag


def as_f32(values):
    return tuple(v.astype(F32) for v in values)


def load_pair(order, core, at, held, pair_ref):
    if len(held) == 1:
        pair_ref[...] = held[0][0]
        return
    if len(held) == 2:
        pair_ref[core] = held[0][0, 0]
        pair_ref[1 - core] = held[1][0, 0]
        return
    for i in range(4):

        @pl.when(order[at] == i)
        def _():
            pair_ref[core] = held[i][...]
            pair_ref[1 - core] = held[4 + i][...]


def load_chunk(counts, refs, order, core, turn, at, pair_ref):
    first = 0
    for k, count in enumerate(counts):

        @pl.when(turn == k)
        def _(held=refs[first : first + count]):
            load_pair(order, core, at, held, pair_ref)

        first += count


def forward_kernel(is_last, counts, stacks, order, scalars, *rest):
    held, (wave_ref, prop_ref, tabs_ref, *rest) = rest[: sum(counts)], rest[sum(counts) :]
    inten_ref, rest = (rest[0], rest[1:]) if is_last else (None, rest)
    out_ref, kept_ref, *stack_refs, pair_ref, lhs_ref, rhs_ref = rest
    step = pl.program_id(0)
    turn, at_z = step // 4, step % 4
    core = scalars[1]
    tabs = [tabs_ref[i] for i in range(4)]

    @pl.when(step == 0)
    def _():
        out_ref[...] = wave_ref[...]

    load_chunk(counts, held, order, core, turn, at_z, pair_ref)
    if stacks:
        stack_refs[0][0, 0] = pair_ref[core]
        stack_refs[1][0, 0] = pair_ref[1 - core]

    def one_slice(j, carry):
        @pl.when((at_z == scalars[0]) & (j == core))
        def _():
            kept_ref[turn] = out_ref[...]

        for at in BLOCKS:
            objr, obji = as_f32(quads_at(pair_ref, (j, 0), at)), as_f32(quads_at(pair_ref, (j, 1), at))
            mixed = times(quads_at(out_ref, (0,), at), quads_at(out_ref, (1,), at), objr, obji)
            for part in (0, 1):
                put_folded(lhs_ref, part, at, fold(*mixed[part]))
        spec = two_sided(lhs_ref, rhs_ref, tabs)
        for at in BLOCKS:
            prop = quads_at(prop_ref, (0,), at), quads_at(prop_ref, (1,), at)
            real, imag = times(*spectrum_rows(spec, at), *prop)
            if is_last:
                final = (step == pl.num_programs(0) - 1) & (j == 1)
                measured = quads_at(inten_ref, (), at)
                scale = [2.0 * (x * x + y * y - z) for x, y, z in zip(real, imag, measured)]
                slope = [[s * x for s, x in zip(scale, values)] for values in (real, imag)]
                back = conj_times(*prop, *slope)
                real, imag = ([jnp.where(final, b, a) for a, b in zip(*pair)] for pair in zip((real, imag), back))
            put_spectrum(lhs_ref, at, real, imag)
        wave = two_sided(lhs_ref, rhs_ref, tabs)
        for at in BLOCKS:
            for part in (0, 1):
                put_quads(out_ref, part, at, unfold(*rows_of(wave, part, at)))
        return carry

    lax.fori_loop(0, 2, one_slice, 0)


def paired_index(shape, axis):
    at = lax.broadcasted_iota(jnp.int32, shape, axis)
    return jnp.where(at < M, at, N + M - 1 - at)


def one_hot(a, b):
    return jnp.where(a == b, 1.0, 0.0).astype(BF16)


def iota(shape, axis):
    return lax.broadcasted_iota(jnp.int32, shape, axis)


def backward_kernel(from_end, counts, order, scalars, *rest):
    chunks = len(counts)
    held, (ct_ref, prop_ref, tabs_ref, *rest) = rest[: sum(counts)], rest[sum(counts) :]
    kept_refs, rest = rest[:chunks], rest[chunks:]
    if from_end:
        out_ref, sent_ref, *rest = rest
    else:
        sent_ref, out_ref, *rest = rest
    grad_ref, mixed_ref, pair_ref, lhs_ref, rhs_ref = rest
    step = pl.program_id(0)
    chunk, at_z = chunks - 1 - step // 4, 3 - step % 4
    core = scalars[1]
    tabs = [tabs_ref[i] for i in range(4)]

    @pl.when(step == 0)
    def _():
        out_ref[...] = ct_ref[...]

    load_chunk(counts, held, order, core, chunk, at_z, pair_ref)

    def one_slice(turn, carry):
        j = 1 - turn

        def put_back(at, mixed):
            objr, obji = as_f32(quads_at(pair_ref, (j, 0), at)), as_f32(quads_at(pair_ref, (j, 1), at))
            back = conj_times(objr, obji, *mixed)
            for part in (0, 1):
                put_quads(mixed_ref, part, at, mixed[part])
                put_quads(out_ref, part, at, back[part])

        def through():
            for at in BLOCKS:
                for part in (0, 1):
                    put_folded(lhs_ref, part, at, fold(*quads_at(out_ref, (part,), at)))
            spec = two_sided(lhs_ref, rhs_ref, tabs)
            for at in BLOCKS:
                prop = quads_at(prop_ref, (0,), at), quads_at(prop_ref, (1,), at)
                put_spectrum(lhs_ref, at, *conj_times(*prop, *spectrum_rows(spec, at)))
            wave = two_sided(lhs_ref, rhs_ref, tabs)
            for at in BLOCKS:
                put_back(at, [unfold(*rows_of(wave, part, at)) for part in (0, 1)])

        if from_end:
            at_end = (step == 0) & (turn == 0)
            pl.when(jnp.logical_not(at_end))(through)

            @pl.when(at_end)
            def _():
                for at in BLOCKS:
                    put_back(at, [quads_at(out_ref, (part,), at) for part in (0, 1)])

        else:
            through()

        for k in range(chunks):

            @pl.when((chunk == k) & (at_z == scalars[0]) & (j == core))
            def _(kept_ref=kept_refs[k]):
                kr, ki, cr, ci = kept_ref[0, 0], kept_ref[0, 1], mixed_ref[0], mixed_ref[1]
                grad_ref[0] = kr * cr + ki * ci
                grad_ref[1] = kr * ci - ki * cr

        return carry

    lax.fori_loop(0, 2, one_slice, 0)

    @pl.when(at_z == 0)
    def _():
        at = iota((N, 1), 0)
        slot = M * ((at >> 3) & 1) + 8 * (at >> 4) + (at & 7)
        rows = one_hot((paired_index((1, N), 1) + scalars[2]) & (N - 1), slot)
        cols = one_hot((paired_index((N, 1), 0) + scalars[3]) & (N - 1), iota((1, N), 1))
        for part in (0, 1):
            high, low = split(grad_ref[part])
            rolled = [dot(rows, dot(x, cols).astype(BF16)) for x in (high, low)]
            sent_ref[:, chunk, part] = (rolled[0] + rolled[1]).reshape(16, 16, N)


def reduce_kernel(count, scalars, tiles_ref, pos_ref, got_ref, out_ref):
    at = iota((16, N), 0)
    slot = M * (at // 8) + 8 * scalars[0] + at % 8
    lane = iota((16, N), 1)
    for part in (0, 1):
        sums = [jnp.zeros((16, N), F32)] * 4
        for p in range(count):
            value = got_ref[p, 0, part]
            held = tiles_ref[p // 4]
            low, wide = slot < pos_ref[held, 0, p % 4], lane < pos_ref[held, 1, p % 4]
            zero = jnp.zeros_like(value)
            below, above = jnp.where(low, value, zero), jnp.where(low, zero, value)
            for i, rows in enumerate((above, below)):
                sums[2 * i] += jnp.where(wide, zero, rows)
                sums[2 * i + 1] += jnp.where(wide, rows, zero)
        for strip in range(4):
            half, fold = strip % 2, strip // 2
            for side in (0, 1):
                out_ref[strip, 0, part, :, side * N : side * N + N] = sums[2 * fold + side][8 * half : 8 * half + 8]


def cut_kernel(rows_ref, cols_ref, starts_ref, *refs):
    blocks, out_ref = refs[:-1], refs[-1]
    strip, width = blocks[0].shape[-2:]
    height = strip * len(blocks)
    at = pl.program_id(0)
    held = jnp.concatenate([iota((1, strip), 1) + starts_ref[i] for i in range(len(blocks))], axis=1)
    rows = one_hot(paired_index((N, 1), 0) + rows_ref[at], held)
    cols = one_hot(paired_index((1, N), 1) + cols_ref[at], iota((width, 1), 0))
    for part in (0, 1):
        whole_part = jnp.concatenate([block[part, 0] for block in blocks], axis=0)
        out_ref[0, part] = dot(dot(rows, whole_part).astype(BF16), cols).astype(BF16)


def whole(shape):
    return pl.BlockSpec(shape, lambda *_: (0,) * len(shape))


SMEM = pl.BlockSpec(memory_space=pltpu.SMEM)
PARAMS = pltpu.CompilerParams(dimension_semantics=("arbitrary",), vmem_limit_bytes=24 << 20)
WAVE = (2, N, N)


def cost(chunks):
    return pl.CostEstimate(flops=chunks * 8 * 32 * N**3, bytes_accessed=chunks << 22, transcendentals=0)


def cut(blocks, starts, pos_rows, pos_cols):
    count = pos_rows.shape[0]
    return pl.pallas_call(
        cut_kernel,
        grid=(count,),
        in_specs=[SMEM] * 3 + [whole(blocks[0].shape)] * len(blocks),
        out_specs=pl.BlockSpec((1, 2, N, N), lambda i: (i, 0, 0, 0)),
        out_shape=jax.ShapeDtypeStruct((count, 2, N, N), BF16),
        compiler_params=PARAMS,
        name="cut",
    )(pos_rows, pos_cols, starts, *blocks)


def chunk_specs(chunks, reverse):
    specs, last = [], len(chunks) - 1
    for k, (blocks, at) in enumerate(chunks):
        if len(blocks) == 8:
            specs += [whole(WAVE)] * 8
            continue

        def block(i, *_, k=k, at=at):
            first = 4 * (last - k if reverse else k)
            inside = jnp.clip(i - first, 0, 3)
            return (3 - inside if reverse else inside, at, 0, 0, 0)

        specs += [pl.BlockSpec((1, 3 - len(blocks), 2, N, N), block)] * len(blocks)
    return specs


def run_forward(order, scalars, chunks, wave, prop, tabs, inten=None, stacks=False):
    counts = [len(blocks) for blocks, _ in chunks]
    last = inten is not None
    extra = (inten,) if last else ()

    def body(*refs):
        forward_kernel(last, counts, stacks, *refs)

    kept = (len(chunks), *WAVE)
    stack = pl.BlockSpec((1, 1, 2, N, N), lambda i, *_: (i, 0, 0, 0, 0))
    return pl.pallas_call(
        body,
        grid_spec=pltpu.PrefetchScalarGridSpec(
            num_scalar_prefetch=2,
            grid=(4 * len(chunks),),
            in_specs=chunk_specs(chunks, False)
            + [whole(WAVE), whole(WAVE), whole((4, N, N))]
            + [whole((N, N))] * len(extra),
            out_specs=[whole(WAVE), whole(kept)] + [stack] * (2 * stacks),
            scratch_shapes=[pltpu.VMEM((2, 2, N, N), BF16)] * 3,
        ),
        out_shape=[jax.ShapeDtypeStruct(WAVE, F32), jax.ShapeDtypeStruct(kept, F32)]
        + [pltpu.HBM((4, 1, 2, N, N), BF16)] * (2 * stacks),
        compiler_params=PARAMS,
        cost_estimate=cost(len(chunks)),
        name="forward",
    )(order, scalars, *in_hbm([x for blocks, _ in chunks for x in blocks]), wave, prop, tabs, *extra)


def run_backward(order, scalars, chunks, ct, prop, tabs, kept, from_end=False):
    counts = [len(blocks) for blocks, _ in chunks]

    def body(*refs):
        backward_kernel(from_end, counts, *refs)

    sent = (16, len(chunks), 2, 16, N)
    return pl.pallas_call(
        body,
        grid_spec=pltpu.PrefetchScalarGridSpec(
            num_scalar_prefetch=2,
            grid=(4 * len(chunks),),
            in_specs=chunk_specs(chunks, True)
            + [whole(WAVE), whole(WAVE), whole((4, N, N))]
            + [pl.BlockSpec((1, *WAVE), lambda *_, at=at: (at, 0, 0, 0)) for _, at in kept],
            out_specs=[whole(WAVE)] * from_end + [whole(sent)],
            scratch_shapes=[pltpu.VMEM(WAVE, F32)] * (3 - from_end) + [pltpu.VMEM((2, 2, N, N), BF16)] * 3,
        ),
        out_shape=[jax.ShapeDtypeStruct(WAVE, F32)] * from_end + [jax.ShapeDtypeStruct(sent, F32)],
        compiler_params=PARAMS,
        cost_estimate=cost(len(chunks)),
        name="backward",
    )(order, scalars, *in_hbm([x for blocks, _ in chunks for x in blocks]), ct, prop, tabs, *[x for x, _ in kept])


def run_reduce(piece, tiles, positions, got):
    sources, count = got.shape[:2]

    def body(*refs):
        reduce_kernel(sources, *refs)

    return pl.pallas_call(
        body,
        grid=(count,),
        in_specs=[SMEM] * 3 + [pl.BlockSpec((sources, 1, 2, 16, N), lambda i: (0, i, 0, 0, 0))],
        out_specs=pl.BlockSpec((4, 1, 2, 8, 2 * N), lambda i: (0, i, 0, 0, 0)),
        out_shape=jax.ShapeDtypeStruct((4, count, 2, 8, 2 * N), F32),
        compiler_params=PARAMS,
        name="reduce",
    )(piece, tiles, positions, got)


def from_neighbour(block, axis, distance):
    size = lax.axis_size(axis)
    return lax.ppermute(block, axis, [(i, (i + distance) % size) for i in range(size)])


def paired(x):
    for axis in (-2, -1):
        first, second = jnp.split(x, 2, axis=axis)
        x = jnp.concatenate([first, jnp.flip(second, axis=axis)], axis=axis)
    return x


def start_wave(probe_wave):
    at = np.arange(N)
    angle = math.pi / N * (at[:, None] + at[None, :])
    cos, sin = np.cos(angle).astype(np.float32), np.sin(angle).astype(np.float32)
    real, imag = probe_wave[0], probe_wave[1]
    return paired(jnp.stack([real * cos - imag * sin, real * sin + imag * cos]))


def around_of(at):
    return (at - jnp.arange(4, dtype=jnp.int32)) % 4


def in_hbm(blocks):
    return [pltpu.with_memory_space_constraint(x, pltpu.HBM) for x in blocks]


def ring_gather(block):
    own = [block] + [from_neighbour(block, "z", d) for d in (1, 2, 3)]
    return own + [from_neighbour(x, "core", 1) for x in own]


def on_device(probe_wave, object_field, pos_rows, pos_cols, intensity, prop_phase):
    row, tile, z, core = (lax.axis_index(name).astype(jnp.int32) for name in ("y", "x", "z", "core"))
    chunks_count = lax.axis_size("y")
    strip, width = object_field.shape[2:]
    moves = (0, 1, 3, 2)
    positions = jnp.stack([pos_rows, pos_cols])
    blocks = [object_field] + [from_neighbour(object_field, "x", d) for d in moves[1:]]
    starts = jnp.stack([(tile - d) % 4 for d in moves]) * strip

    *tabs, gain = tables()
    tabs = jnp.asarray(np.stack(tabs))
    prop = paired(jnp.stack([jnp.cos(prop_phase), jnp.sin(prop_phase)]) * (1.0 / gain))
    inten = paired(lax.dynamic_index_in_dim(intensity, row, 0, keepdims=False))
    wave = start_wave(probe_wave)
    scalars = jnp.stack([z, core, pos_rows[row], pos_cols[row]])
    patches = cut(blocks, starts, pos_rows, pos_cols)
    patches, positions = lax.optimization_barrier((patches, positions))
    positions = jnp.stack([positions] + [from_neighbour(positions, "x", d) for d in (1, 2, 3)])
    patches = lax.all_to_all(patches, "y", 0, 0, tiled=True)
    small = (positions, prop, inten, wave, scalars)
    patches, (positions, prop, inten, wave, scalars) = lax.optimization_barrier((patches, small))
    first, patches = lax.optimization_barrier((patches[0], patches))
    middle = lax.all_gather(patches[1:3], "z", axis=0)
    final = lax.all_gather(patches[3:], ("z", "core"), axis=0)
    order = around_of(z)

    def forward(chunks, wave, **more):
        return run_forward(order, scalars, chunks, wave, prop, tabs, **more)

    wave, kept0, *stacked = forward([(ring_gather(first), 0)], wave, stacks=True)
    middle, wave = lax.optimization_barrier((middle, wave))
    middle = [middle, from_neighbour(middle, "core", 1)]
    wave, kept12 = forward([(middle, 0), (middle, 1)], wave)
    final, wave = lax.optimization_barrier((final, wave))
    final = [final.reshape(4, 2, *WAVE)]
    wave, kept3 = forward([(final, 0)], wave, inten=inten)

    def backward(chunks, wave, kept, **more):
        return run_backward(order, scalars, chunks, wave, prop, tabs, kept, **more)

    wave, sent23 = backward([(middle, 1), (final, 0)], wave, [(kept12, 1), (kept3, 0)], from_end=True)
    got23 = lax.all_to_all(sent23, ("x", "y"), 0, 0, tiled=True)
    (sent01,) = backward([(stacked, 0), (middle, 0)], wave, [(kept0, 0), (kept12, 0)])
    got23, sent01 = lax.optimization_barrier((got23, sent01))
    got01 = lax.all_to_all(sent01, ("x", "y"), 0, 0, tiled=True)
    got = [got01, got23]
    piece = (tile * 4 + row)[None]
    sums = [run_reduce(piece, around_of(tile), positions, x) for x in got]
    sums = jnp.concatenate(sums, axis=1).reshape(16, 2, 8, width)
    out = lax.all_to_all(sums, ("x", "y"), 0, 0, tiled=True)
    return jnp.transpose(out, (1, 0, 2, 3)).reshape(2, 1, strip, width)


def solution(mesh):
    devices = mesh.devices
    fine = Mesh(devices.reshape(4, 4, 2, devices.shape[1]), ("y", "z", "core", "x"))
    cuts = ("y", "z", "core")
    return jax.shard_map(
        on_device,
        mesh=fine,
        in_specs=(
            P(),
            P(None, cuts, "x", None),
            P("x"),
            P("x"),
            P("x", None, None),
            P(),
        ),
        out_specs=P(None, cuts, "x", None),
        check_vma=False,
    )
```
